256 devices in a mesh: blk: 16 (over x, z_lo, core), tp: 16 (over y, z_hi).
Axes of the slice: x: 4, y: 4, z: 8 (z_hi: 4, z_lo: 2; z = z_hi * 2 + z_lo), core: 2. Of those that a mesh axis runs over, the one named last changes fastest.
Arguments:
- residual_in: bfloat16 [8192, 5120], P('blk'), may hold values from -6 to 6
- norm_gain: bfloat16 [5120], replicated, may hold values from 0.099609375 to 1.8984375
- w_query: bfloat16 [5120, 4096], P(('blk', 'tp')), may hold values from -0.5 to 0.5
- w_key_value: bfloat16 [5120, 2048], P(('blk', 'tp')), may hold values from -0.5 to 0.5
- query_bias: bfloat16 [4096], replicated, may hold values from -3 to 3
- key_value_bias: bfloat16 [2048], replicated, may hold values from -3 to 3
- w_output: bfloat16 [4096, 5120], P(None, ('blk', 'tp')), may hold values from -0.09375 to 0.09375
- device_map: int32 [256], replicated, may hold values from 0 to 255, each once
- positions: int32 [8192], P('blk'), may hold values from 0 to 10238, as said below
- segments: int32 [8192], P('blk'), may hold values from 0 to 1, as said below
Outputs:
- output: bfloat16 [8192, 5120], P('blk', 'tp')
The draws below stay inside these ranges and needn't reach their ends.
Inputs may be any that keep to these rules, and one draw needn't show every extreme that they name: `segments`: ids never fall; both ids 0 and 1 occur; the shorter prompt holds a quarter of 512 up to 511 tokens. `positions`: a token's index within its prompt plus an offset shared by the whole prompt; the longer prompt's last token stands at 10238. `device_map`: each of 0 to 255 once.
All inputs are finite; a program needn't handle non-finite values.
Results may differ from the reference program's by a relative error of at most 0.012.
Values may be sent and summed in bfloat16 or wider, within the bound.
A program may use at most 64 MiB of HBM per device.

```python
import jax
import jax.numpy as jnp
from jax import lax

D = 5120
HEADS = 32
KVH = 8
HD = 128
TOK_DEV = 512
LEN = 8192
QW = 4096
KVW = 2048
TRAINER_ROWS = 20
DEVICES = 256


def weight_pair(key):
    base_key = jax.random.fold_in(key, 11)
    query_key, pair_key = jax.random.split(base_key, 2)
    query_raw = jnp.clip(jax.random.normal(query_key, (D, KVH, HEADS // KVH, HD), jnp.float32), -6.0, 6.0)
    pairs_raw = jnp.clip(jax.random.normal(pair_key, (D, KVH, 2, HD), jnp.float32), -6.0, 6.0)
    fan_scale = D ** (-0.5)
    query_scaled = jnp.clip(query_raw.reshape(D, HEADS * HD) * fan_scale, -0.5, 0.5)
    pairs_scaled = jnp.clip(pairs_raw.reshape(D, 2 * KVH * HD) * fan_scale, -0.5, 0.5)
    return (query_scaled.astype(jnp.bfloat16), pairs_scaled.astype(jnp.bfloat16))


def prompt_layout(key):
    base_key = jax.random.fold_in(key, 23)
    short_key, order_key, offset_key = jax.random.split(base_key, 3)
    short_len = jax.random.randint(short_key, (), TOK_DEV // 4, TOK_DEV)
    first_short = jax.random.randint(order_key, (), 0, 2)
    boundary = jnp.where(first_short == 1, short_len, LEN - short_len)
    index_all = jnp.arange(LEN, dtype=jnp.int32)
    segment_ids = (index_all >= boundary).astype(jnp.int32)
    short_offset = jax.random.randint(offset_key, (), 0, 2048)
    long_offset = short_len + 2047
    offset_zero = jnp.where(first_short == 1, short_offset, long_offset)
    offset_one = jnp.where(first_short == 1, long_offset, short_offset)
    starts = jnp.where(segment_ids == 1, boundary, 0)
    shifted = jnp.where(segment_ids == 1, offset_one, offset_zero)
    return (segment_ids, (index_all - starts + shifted).astype(jnp.int32))


def draw_w_query(key, part):
    return weight_pair(key)[0]


def draw_w_key_value(key, part):
    return weight_pair(key)[1]


def draw_segments(key, part):
    return prompt_layout(key)[0]


def draw_positions(key, part):
    return prompt_layout(key)[1]


def level_of(own_key, extent, cuts, low, high):
    level, own = 1.0, jax.random.fold_in(own_key, 6)
    for position, shards_of in cuts:
        steps = jnp.exp(jax.random.uniform(jax.random.fold_in(own, position), (shards_of,), jnp.float32, low / len(cuts), high / len(cuts)))
        level = level * jnp.repeat(steps, extent[position] // shards_of).reshape([-1 if axis == position else 1 for axis in range(len(extent))])
    return level


def noise(key, extent, scale, limit, cuts=(), held_as=jnp.bfloat16):
    result = scale * jax.random.normal(key, extent, jnp.float32)
    if cuts:
        result = result * level_of(key, extent, cuts, -0.22, 0.18)
    return jnp.clip(result, -limit, limit).astype(held_as)


def setup_inputs(seed: int = 0) -> dict:
    splits = jax.random.split(jax.random.key(seed), 11)
    residual_in = noise(splits[0], (LEN, D), 1.0, 6.0, ((0, 16),))
    norm_gain = jnp.clip(1.0 + 0.18 * jax.random.normal(splits[1], (D,), jnp.float32), 0.099609375, 1.8984375).astype(jnp.bfloat16)
    w_query = draw_w_query(jax.random.fold_in(splits[10], 71), 0)
    w_key_value = draw_w_key_value(jax.random.fold_in(splits[10], 71), 0)
    query_bias = noise(splits[4], (QW,), 0.5, 3.0)
    key_value_bias = noise(splits[5], (KVW,), 0.5, 3.0)
    w_output = noise(splits[6], (QW, D), QW ** -0.5, 0.09375, ((1, 256),))
    device_map = jax.random.permutation(splits[7], DEVICES).astype(jnp.int32)
    positions = draw_positions(jax.random.fold_in(splits[10], 71), 0)
    segments = draw_segments(jax.random.fold_in(splits[10], 71), 0)
    return {"residual_in": residual_in, "norm_gain": norm_gain, "w_query": w_query, "w_key_value": w_key_value, "query_bias": query_bias, "key_value_bias": key_value_bias, "w_output": w_output, "device_map": device_map, "positions": positions, "segments": segments}


NORM_FLOOR = 0.0625
ROPE_BASE = 1000000.0
NEGATIVE_FILL = -1e+30

def rope_tables(positions, head_width):
    half_width = head_width // 2
    frequency = ROPE_BASE ** (-(jnp.arange(half_width, dtype=jnp.float32) * 2.0) / head_width)
    angles = positions.astype(jnp.float32)[:, None] * frequency[None, :]
    angles = jnp.concatenate([angles, angles], axis=1)
    return (jnp.cos(angles), jnp.sin(angles))

def rotate(values, cosine_table, sine_table):
    half_width = values.shape[-1] // 2
    turned = jnp.concatenate([-values[..., half_width:], values[..., :half_width]], axis=-1)
    return values * cosine_table[:, None, :] + turned * sine_table[:, None, :]

def reference(residual_in, norm_gain, w_query, w_key_value, query_bias, key_value_bias, w_output, device_map, positions, segments):
    floats = residual_in.astype(jnp.float32)
    square = jnp.maximum(lax.optimization_barrier(jnp.mean(floats * floats, axis=1, keepdims=True)), NORM_FLOOR)
    normed = (floats * lax.rsqrt(square) * norm_gain.astype(jnp.float32)).astype(jnp.bfloat16)
    ordered = jnp.take(normed.reshape(LEN, DEVICES, TRAINER_ROWS), device_map, axis=1).reshape(LEN, D)
    queries = jnp.dot(ordered, w_query, preferred_element_type=jnp.float32) + query_bias.astype(jnp.float32)
    key_value = jnp.dot(ordered, w_key_value, preferred_element_type=jnp.float32) + key_value_bias.astype(jnp.float32)
    cosine_table, sine_table = rope_tables(positions, HD)
    query_rot = rotate(queries.reshape(LEN, HEADS, HD), cosine_table, sine_table).astype(jnp.bfloat16)
    paired = key_value.reshape(LEN, KVH, 2, HD)
    key_rot = rotate(paired[:, :, 0, :], cosine_table, sine_table).astype(jnp.bfloat16)
    values = paired[:, :, 1, :].astype(jnp.bfloat16)
    per_group = HEADS // KVH
    query_rows = min(512, LEN)
    attend_scale = HD ** (-0.5)
    key_index = jnp.arange(LEN, dtype=jnp.int32)

    def one_block(block_number):
        block_start = (block_number * query_rows).astype(jnp.int32)
        query_block = lax.dynamic_slice_in_dim(query_rot, block_start, query_rows, 0)
        query_segment = lax.dynamic_slice_in_dim(segments, block_start, query_rows, 0)
        row_index = block_start + jnp.arange(query_rows, dtype=jnp.int32)
        visible = (key_index[None, :] <= row_index[:, None]) & (segments[None, :] == query_segment[:, None])

        def one_group(group_number):
            group_start = (group_number * per_group).astype(jnp.int32)
            query_group = lax.dynamic_slice_in_dim(query_block, group_start, per_group, 1).astype(jnp.float32)
            key_group = lax.dynamic_index_in_dim(key_rot, group_number, 1, keepdims=False).astype(jnp.float32)
            value_group = lax.dynamic_index_in_dim(values, group_number, 1, keepdims=False).astype(jnp.float32)
            scores = jnp.einsum('qhd,kd->hqk', query_group, key_group, precision=lax.Precision.HIGHEST) * attend_scale
            masked = jnp.where(visible[None], scores, NEGATIVE_FILL)
            row_peak = lax.optimization_barrier(jnp.max(masked, axis=2, keepdims=True))
            raw_weights = jnp.where(visible[None], jnp.exp(masked - row_peak), 0.0)
            weights = lax.optimization_barrier(raw_weights.astype(jnp.bfloat16)).astype(jnp.float32)
            context = jnp.einsum('hqk,kd->hqd', weights, value_group, precision=lax.Precision.HIGHEST)
            context = context / lax.optimization_barrier(jnp.sum(raw_weights, axis=2, keepdims=True))
            return context.astype(jnp.bfloat16)
        grouped = lax.map(one_group, jnp.arange(KVH, dtype=jnp.int32))
        return grouped.transpose(2, 0, 1, 3).reshape(query_rows, QW)
    blocks_out = lax.map(one_block, jnp.arange(LEN // query_rows, dtype=jnp.int32))
    context = blocks_out.reshape(LEN, QW)
    mixed = jnp.dot(context, w_output, preferred_element_type=jnp.float32)
    return (residual_in.astype(jnp.float32) + mixed).astype(jnp.bfloat16)
```

```python
import functools

import jax
import jax.numpy as jnp
from jax import lax
from jax.experimental import pallas as pl
from jax.experimental.pallas import tpu as pltpu
from jax.sharding import PartitionSpec as P

D = 5120
HD = 128
TOK = 512
ROWS = 20
NORM_FLOOR = 0.0625
ROPE_BASE = 1000000.0
NEGATIVE_FILL = -1e30
LOG2E = 1.4426950408889634
MESH = pl.DeviceIdType.MESH
VM = pltpu.VMEM
BF = jnp.bfloat16
F32 = jnp.float32
VLIM = 62 * 1024 * 1024


def coords():
    b = lax.axis_index("blk")
    t = lax.axis_index("tp")
    x = b // 4
    zl = (b // 2) % 2
    c = b % 2
    y = t // 4
    zh = t % 4
    return b, t, x, zl, c, y, zh


def blk_of(x, zl, c):
    return x * 4 + zl * 2 + c


def signal(dev):
    pl.semaphore_signal(pltpu.get_barrier_semaphore(), inc=1, device_id=dev, device_id_type=MESH)


def push(src, dst, ssem, rsem, dev):
    pltpu.make_async_remote_copy(src, dst, ssem, rsem, device_id=dev, device_id_type=MESH).start()


class Gather:
    def __init__(self, at, pieces, send, recv):
        self.at, self.n, self.send, self.recv = at, pieces, send, recv
        b, t, x, zl, c, y, zh = coords()
        self.t = t
        self.own = b
        self.sib = blk_of(x, zl, 1 - c)
        self.z = blk_of(x, 1 - zl, c)
        xp, xm, x2 = (x + 1) % 4, (x + 3) % 4, (x + 2) % 4
        self.xp, self.xm = blk_of(xp, zl, c), blk_of(xm, zl, c)
        self.xpz, self.xmz = blk_of(xp, 1 - zl, c), blk_of(xm, 1 - zl, c)
        self.x2, self.x2z = blk_of(x2, zl, c), blk_of(x2, 1 - zl, c)
        self.count = 0
        self.sent = []

    def peers(self):
        return [self.sib, self.z, self.xp, self.xm]

    def _send(self, chunk, p, to):
        ref = self.at(chunk, p)
        k = self.count
        self.count += 1
        push(ref, ref, self.send.at[k], self.recv.at[chunk, p], {"blk": to, "tp": self.t})
        self.sent.append((chunk, p, k))

    def wait(self, chunk, p):
        ref = self.at(chunk, p)
        pltpu.make_async_copy(ref, ref, self.recv.at[chunk, p]).wait()

    def own_piece(self, p):
        for to in (self.xp, self.xm, self.z, self.sib):
            self._send(self.own, p, to)

    def z_piece(self, p):
        self.wait(self.z, p)
        for to in (self.xp, self.xm, self.sib):
            self._send(self.z, p, to)

    def side(self, p, zside):
        minus, plus = (self.xmz, self.xpz) if zside else (self.xm, self.xp)
        half = self.n // 2
        self.wait(minus, p)
        if p < half:
            self._send(minus, p, self.xp)
        self._send(minus, p, self.sib)
        self.wait(plus, p)
        if p >= half:
            self._send(plus, p, self.xm)
        self._send(plus, p, self.sib)

    def far(self, p, zside):
        chunk = self.x2z if zside else self.x2
        self.wait(chunk, p)
        self._send(chunk, p, self.sib)

    def forward_all(self):
        for p in range(self.n):
            self.z_piece(p)
        for zside in (False, True):
            for p in range(self.n):
                self.side(p, zside)
        for zside in (False, True):
            for p in range(self.n):
                self.far(p, zside)

    def sibling_chunks(self):
        flip = lambda k: k + 1 - 2 * (k % 2)
        return [flip(k) for k in (self.own, self.z, self.xm, self.xp, self.xmz, self.xpz, self.x2, self.x2z)]

    def wait_sibling(self):
        for chunk in self.sibling_chunks():
            for p in range(self.n):
                self.wait(chunk, p)

    def drain(self):
        for chunk, p, k in self.sent:
            ref = self.at(chunk, p)
            pltpu.make_async_copy(ref, ref, self.send.at[k]).wait()


def sends_of(pieces):
    return 15 * pieces


def prep_kernel(dm, x_ref, gain_ref, out_ref, slot, five):
    acc = jnp.zeros((TOK, 128), F32)
    for j in range(D // 128):
        v = x_ref[:, j * 128 : (j + 1) * 128].astype(F32)
        acc = acc + v * v
    square = jnp.maximum(jnp.sum(acc, axis=1, keepdims=True) * (1.0 / D), NORM_FLOOR)
    scale = lax.rsqrt(square)

    def turn(i, carry):
        for k in range(5):
            at = pl.ds(pl.multiple_of(i * 640 + k * 128, 128), 128)
            v = x_ref[:, at].astype(F32) * scale * gain_ref[:, at].astype(F32)
            five[k * 128 : (k + 1) * 128, :] = v.astype(BF).astype(F32).T
        for k in range(32):
            slot[i * 32 + k] = five[k * ROWS : (k + 1) * ROWS, :]
        return carry

    lax.fori_loop(0, 8, turn, 0)

    def back(i, carry):
        for k in range(32):
            five[k * ROWS : (k + 1) * ROWS, :] = slot[dm[i * 32 + k]]
        for k in range(5):
            at = pl.ds(pl.multiple_of(i * 640 + k * 128, 128), 128)
            out_ref[:, at] = five[k * 128 : (k + 1) * 128, :].T.astype(BF)
        return carry

    lax.fori_loop(0, 8, back, 0)


def prep(x, gain, device_map):
    return pl.pallas_call(
        prep_kernel,
        out_shape=jax.ShapeDtypeStruct((TOK, D), BF),
        in_specs=[pl.BlockSpec(memory_space=pltpu.SMEM), pl.BlockSpec(memory_space=VM), pl.BlockSpec(memory_space=VM)],
        out_specs=pl.BlockSpec(memory_space=VM),
        scratch_shapes=[VM((256, ROWS, TOK), F32), VM((640, TOK), F32)],
        compiler_params=pltpu.CompilerParams(vmem_limit_bytes=VLIM),
        name="prep",
    )(device_map, x, gain.reshape(1, D))


def weights_kernel(
    wq, wkv, wo, seg, ordered, bias, cos, sin, qseg,
    q_out, kv_out, wo_out, seg_out,
    land, wide, w, land_o, wide_o, wog,
    a_send, a_recv, o_send, o_recv, s_send, s_recv, g_send, g_recv, h_send, h_recv, l_sem,
):
    b, t, x, zl, c, y, zh = coords()
    main = Gather(lambda k, p: w.at[k, pl.ds(p * 80, 80)], 4, g_send, g_recv)
    outw = Gather(lambda k, p: wog.at[k, :, pl.ds(p * 512, 512)], 2, h_send, h_recv)
    tgt_blk = blk_of(x, y // 2, y % 2)
    tgt_tp = [yb * 4 + 2 * zl + c for yb in range(4)]
    src_blk = blk_of(x, zh // 2, zh % 2)
    src_tp = [(2 * zl + c) * 4 + k for k in range(4)]

    def other(kb, kt):
        return jnp.logical_or(kb != b, kt != t)

    for k in range(1, 16):
        signal({"blk": b, "tp": (t + k) % 16})
        signal({"blk": (b + k) % 16, "tp": t})
    for k in range(4):
        @pl.when(other(tgt_blk, tgt_tp[k]))
        def _():
            signal({"blk": tgt_blk, "tp": tgt_tp[k]})

        @pl.when(other(src_blk, src_tp[k]))
        def _():
            signal({"blk": src_blk, "tp": src_tp[k]})
    loop = jnp.logical_and(y == 2 * zl + c, zh == 2 * zl + c).astype(jnp.int32)
    pl.semaphore_wait(pltpu.get_barrier_semaphore(), 38 - 2 * loop)

    def q_src(to):
        return wq.at[:, pl.ds(pl.multiple_of(to * 256, 256), 256)]

    def kv_src(to):
        return wkv.at[:, pl.ds(pl.multiple_of((to // 2) * 256, 256), 256)]

    def q_land(k):
        return land.at[k, :, pl.ds(0, 256)]

    def kv_land(k):
        return land.at[k, :, pl.ds(256, 256)]

    order = [4, 12, 1, 3, 5, 7, 13, 15, 8, 2, 9, 6, 14, 10, 11]
    for k in order:
        to = (t + k) % 16
        push(q_src(to), q_land(t), a_send.at[0, k], a_recv.at[0, t], {"blk": b, "tp": to})
        push(kv_src(to), kv_land(t), a_send.at[1, k], a_recv.at[1, t], {"blk": b, "tp": to})
    pltpu.make_async_copy(q_src(t), q_land(t), a_recv.at[0, t]).start()
    pltpu.make_async_copy(kv_src(t), kv_land(t), a_recv.at[1, t]).start()
    for k in range(1, 16):
        push(seg, seg_out.at[b], s_send.at[k], s_recv.at[b], {"blk": (b + k) % 16, "tp": t})
    pltpu.make_async_copy(seg, seg_out.at[b], s_recv.at[b]).start()
    for k in range(4):
        src = wo.at[:, pl.ds(k * 1024, 1024)]

        @pl.when(other(tgt_blk, tgt_tp[k]))
        def _():
            push(src, land_o.at[zh], o_send.at[k], o_recv.at[zh], {"blk": tgt_blk, "tp": tgt_tp[k]})

        @pl.when(jnp.logical_not(other(tgt_blk, tgt_tp[k])))
        def _():
            pltpu.make_async_copy(src, land_o.at[zh], o_recv.at[zh]).start()

    for g in range(4):
        for k in range(4 * g, 4 * g + 4):
            pltpu.make_async_copy(q_src(0), q_land(k), a_recv.at[0, k]).wait()
            pltpu.make_async_copy(kv_src(0), kv_land(k), a_recv.at[1, k]).wait()
            wide[pl.ds(k * ROWS, ROWS), :] = land[k].astype(F32)
        w[b, pl.ds(g * 80, 80), :] = wide[pl.ds(g * 80, 80), :].astype(BF)
        main.own_piece(g)
    main.forward_all()
    for k in range(4):
        pltpu.make_async_copy(wo.at[:, pl.ds(0, 1024)], land_o.at[k], o_recv.at[k]).wait()
        wide_o[pl.ds(k * ROWS, ROWS), :] = land_o[k].astype(F32)
    wog[b] = wide_o[...].astype(BF)
    for p in range(2):
        outw.own_piece(p)
    main.wait_sibling()

    half = TOK // 2
    for r in range(2):
        rows = pl.ds(r * half, half)
        v = jnp.dot(ordered[rows, :], w[...].reshape(D, 512), preferred_element_type=F32) + bias[...]
        cs, sn = cos[rows, :], sin[rows, :]
        for h in range(3):
            u = v[:, h * HD : (h + 1) * HD]
            rot = u * cs + pltpu.roll(u, HD // 2, 1) * sn
            if h < 2:
                q_out[h, rows, 0:HD] = rot.astype(BF)
                q_out[h, rows, HD : 2 * HD] = qseg[rows, :]
            else:
                kv_out[rows, 0:HD] = rot.astype(BF)
        kv_out[rows, HD : 2 * HD] = v[:, 3 * HD :].astype(BF)
    outw.forward_all()
    outw.wait_sibling()
    wo_out[...] = wog[...]
    for k in range(16):
        pltpu.make_async_copy(seg, seg_out.at[k], s_recv.at[k]).wait()
    for k in range(1, 16):
        pltpu.make_async_copy(q_src(0), q_land(0), a_send.at[0, k]).wait()
        pltpu.make_async_copy(kv_src(0), kv_land(0), a_send.at[1, k]).wait()
        pltpu.make_async_copy(seg, seg_out.at[0], s_send.at[k]).wait()
    for k in range(4):
        @pl.when(other(tgt_blk, tgt_tp[k]))
        def _():
            pltpu.make_async_copy(wo.at[:, pl.ds(0, 1024)], land_o.at[k], o_send.at[k]).wait()
    main.drain()
    outw.drain()


def weights(wq, wkv, wo, seg, ordered, bias, cos, sin, qseg):
    hbm = pl.BlockSpec(memory_space=pl.ANY)
    vm = pl.BlockSpec(memory_space=VM)
    dma = pltpu.SemaphoreType.DMA
    return pl.pallas_call(
        weights_kernel,
        out_shape=(
            jax.ShapeDtypeStruct((2, TOK, 256), BF),
            jax.ShapeDtypeStruct((TOK, 256), BF),
            jax.ShapeDtypeStruct((16, 80, 1024), BF),
            jax.ShapeDtypeStruct((16, 1, TOK), jnp.int32),
        ),
        in_specs=[hbm, hbm, hbm, vm, vm, vm, vm, vm, vm],
        out_specs=(vm, vm, vm, vm),
        scratch_shapes=[
            VM((16, ROWS, 512), BF),
            VM((320, 512), F32),
            VM((16, 320, 512), BF),
            VM((4, ROWS, 1024), BF),
            VM((80, 1024), F32),
            VM((16, 80, 1024), BF),
            dma((2, 16)), dma((2, 16)), dma((4,)), dma((4,)), dma((16,)), dma((16,)),
            dma((sends_of(4),)), dma((16, 4)), dma((sends_of(2),)), dma((16, 2)), dma((2,)),
        ],
        compiler_params=pltpu.CompilerParams(collective_id=0, has_side_effects=True, vmem_limit_bytes=VLIM),
        name="weights",
    )(wq, wkv, wo, seg, ordered, bias, cos, sin, qseg)


def attend_kernel(q, kv, kaug, ctx, kvg, m_s, acc_s, g_send, g_recv):
    b, t, x, zl, c, y, zh = coords()
    gather = Gather(lambda k, p: kvg.at[k, pl.ds(p * 128, 128)], 4, g_send, g_recv)
    peers = gather.peers()
    for k in peers:
        signal({"blk": k, "tp": t})
    pl.semaphore_wait(pltpu.get_barrier_semaphore(), 4)
    kvg[b] = kv[...]
    for p in range(4):
        gather.own_piece(p)
    coef = HD ** -0.5 * LOG2E
    half = TOK // 2

    def block(j, diagonal):
        kop = jnp.concatenate([kvg[j, :, 0:HD], kaug[j]], axis=1)
        vop = jnp.concatenate([kvg[j, :, HD:], jnp.ones((TOK, HD), BF)], axis=1)
        for h in range(2):
            for r in range(2):
                rows = pl.ds(r * half, half)
                s = lax.dot_general(q[h, rows, :], kop, (((1,), (1,)), ((), ())), preferred_element_type=F32)
                if diagonal:
                    qi = lax.broadcasted_iota(jnp.int32, s.shape, 0) + r * half
                    ki = lax.broadcasted_iota(jnp.int32, s.shape, 1)
                    s = jnp.where(ki <= qi, s, NEGATIVE_FILL)
                peak = jnp.max(s, axis=1, keepdims=True)
                if diagonal:
                    new = peak
                else:
                    old = m_s[h, rows, :]
                    new = jnp.maximum(old, peak)
                    factor = jnp.exp2((old - new) * coef)
                e = jnp.exp2(s * coef - (new * coef)[:, 0:1]).astype(BF)
                o = jnp.dot(e, vop, preferred_element_type=F32)
                if diagonal:
                    m_s[h, rows, :] = jnp.broadcast_to(new, (half, HD))
                    acc_s[h, rows, :] = o
                else:
                    m_s[h, rows, :] = new
                    acc_s[h, rows, 0:HD] = acc_s[h, rows, 0:HD] * factor + o[:, 0:HD]
                    acc_s[h, rows, HD:] = acc_s[h, rows, HD:] * factor + o[:, HD:]

    block(b, True)
    gather.forward_all()
    gather.wait_sibling()

    def body(j, carry):
        block(j, False)
        return carry

    lax.fori_loop(0, b, body, 0)
    for h in range(2):
        ctx[:, h * HD : (h + 1) * HD] = (acc_s[h, :, 0:HD] / acc_s[h, :, HD:]).astype(BF)
    gather.drain()


def attend(q, kv, kaug):
    vm = pl.BlockSpec(memory_space=VM)
    dma = pltpu.SemaphoreType.DMA
    return pl.pallas_call(
        attend_kernel,
        out_shape=jax.ShapeDtypeStruct((TOK, 256), BF),
        in_specs=[vm, vm, vm],
        out_specs=vm,
        scratch_shapes=[
            VM((16, TOK, 256), BF),
            VM((2, TOK, HD), F32),
            VM((2, TOK, 2 * HD), F32),
            dma((sends_of(4),)), dma((16, 4)),
        ],
        compiler_params=pltpu.CompilerParams(collective_id=1, has_side_effects=True, vmem_limit_bytes=VLIM),
        name="attend",
    )(q, kv, kaug)


def out_kernel(ctx, wo, res, out, cg, far, plus, minus, r_far, r_plus, r_minus, c_send, c_recv, p_send, p_recv):
    b, t, x, zl, c, y, zh = coords()
    up, down, opp = (zh + 1) % 4, (zh + 3) % 4, (zh + 2) % 4
    yp, ym, y2 = (y + 1) % 4, (y + 3) % 4, (y + 2) % 4
    zdev = lambda k: {"blk": b, "tp": y * 4 + k}
    ydev = lambda k: {"blk": b, "tp": k * 4 + zh}
    for dev in (zdev(up), zdev(down), ydev(yp), ydev(ym)):
        signal(dev)
    pl.semaphore_wait(pltpu.get_barrier_semaphore(), 4)
    cg[zh] = ctx[...]
    at = lambda k, p: cg.at[k, pl.ds(p * 256, 256)]

    def waitc(k, p):
        pltpu.make_async_copy(at(k, p), at(k, p), c_recv.at[k, p]).wait()

    for p in range(2):
        push(at(zh, p), at(zh, p), c_send.at[p], c_recv.at[zh, p], zdev(up))
        push(at(zh, 1 - p), at(zh, 1 - p), c_send.at[2 + p], c_recv.at[zh, 1 - p], zdev(down))
    waitc(down, 0)
    push(at(down, 0), at(down, 0), c_send.at[4], c_recv.at[down, 0], zdev(up))
    waitc(up, 1)
    push(at(up, 1), at(up, 1), c_send.at[5], c_recv.at[up, 1], zdev(down))
    waitc(down, 1)
    waitc(up, 0)
    waitc(opp, 0)
    waitc(opp, 1)

    def partial(k):
        rows = pl.ds(pl.multiple_of(k * 320, 64), 320)
        v = jnp.zeros((320, TOK), F32)
        for i in range(4):
            v = v + lax.dot_general(
                wo[rows, i * 256 : (i + 1) * 256], cg[i], (((1,), (1,)), ((), ())), preferred_element_type=F32
            )
        return v

    far[...] = partial(y2).astype(BF)
    lo, hi = pl.ds(0, 160), pl.ds(160, 160)
    push(far.at[lo], r_far.at[lo], p_send.at[0], p_recv.at[0], ydev(yp))
    push(far.at[hi], r_far.at[hi], p_send.at[1], p_recv.at[1], ydev(ym))
    v = partial(yp)
    plus[hi, :] = v[160:].astype(BF)
    push(plus.at[hi], r_plus.at[hi], p_send.at[2], p_recv.at[2], ydev(yp))
    u = partial(ym)
    minus[lo, :] = u[:160].astype(BF)
    push(minus.at[lo], r_minus.at[lo], p_send.at[3], p_recv.at[3], ydev(ym))
    pltpu.make_async_copy(far.at[lo], r_far.at[lo], p_recv.at[0]).wait()
    plus[lo, :] = (v[:160] + r_far[lo, :].astype(F32)).astype(BF)
    push(plus.at[lo], r_plus.at[lo], p_send.at[4], p_recv.at[4], ydev(yp))
    pltpu.make_async_copy(far.at[hi], r_far.at[hi], p_recv.at[1]).wait()
    minus[hi, :] = (u[160:] + r_far[hi, :].astype(F32)).astype(BF)
    push(minus.at[hi], r_minus.at[hi], p_send.at[5], p_recv.at[5], ydev(ym))
    mine = partial(y) + res[...].astype(F32)
    for half, k1, k2 in ((hi, 2, 5), (lo, 4, 3)):
        pltpu.make_async_copy(plus.at[half], r_plus.at[half], p_recv.at[k1]).wait()
        pltpu.make_async_copy(minus.at[half], r_minus.at[half], p_recv.at[k2]).wait()
    out[...] = (mine + r_plus[...].astype(F32) + r_minus[...].astype(F32)).astype(BF)
    for k in range(6):
        pltpu.make_async_copy(at(0, 0), at(0, 0), c_send.at[k]).wait()
        pltpu.make_async_copy(far.at[lo], r_far.at[lo], p_send.at[k]).wait()


def project(ctx, wo, res):
    vm = pl.BlockSpec(memory_space=VM)
    dma = pltpu.SemaphoreType.DMA
    return pl.pallas_call(
        out_kernel,
        out_shape=jax.ShapeDtypeStruct((320, TOK), BF),
        in_specs=[vm, vm, vm],
        out_specs=vm,
        scratch_shapes=[VM((4, TOK, 256), BF)] + [VM((320, TOK), BF)] * 6
        + [dma((6,)), dma((4, 2)), dma((6,)), dma((6,))],
        compiler_params=pltpu.CompilerParams(collective_id=2, has_side_effects=True, vmem_limit_bytes=VLIM),
        name="project",
    )(ctx, wo, res)


def per_device(residual_in, norm_gain, w_query, w_key_value, query_bias, key_value_bias, w_output, device_map, positions, segments):
    t = lax.axis_index("tp")
    ordered = prep(residual_in, norm_gain, device_map)
    frequency = ROPE_BASE ** (-(jnp.arange(HD // 2, dtype=F32) * 2.0) / HD)
    angles = positions.astype(F32)[:, None] * frequency[None, :]
    cos, sin = jnp.cos(angles), jnp.sin(angles)
    cos = jnp.concatenate([cos, cos], axis=1)
    sin = jnp.concatenate([-sin, sin], axis=1)
    bias = jnp.concatenate(
        [
            lax.dynamic_slice_in_dim(query_bias, t * 256, 256),
            lax.dynamic_slice_in_dim(key_value_bias, (t // 2) * 256, 256),
        ]
    ).astype(F32)[None, :]
    lane = jnp.arange(HD, dtype=jnp.int32)[None, :] == 0
    qseg = jnp.where(lane, segments[:, None], 0).astype(BF)
    q, kv, wo, segs = weights(w_query, w_key_value, w_output.T, segments[None, :], ordered, bias, cos, sin, qseg)
    kaug = jnp.where(lane[None], jnp.where(segs.reshape(16, TOK, 1) == 0, NEGATIVE_FILL, 0.0), 0.0).astype(BF)
    ctx = attend(q, kv, kaug)
    res = lax.dynamic_slice_in_dim(residual_in, t * 320, 320, 1).T
    return project(ctx, wo.reshape(1280, 1024), res).T


def solution(mesh):
    both = ("blk", "tp")
    placed = (P("blk", None), P(), P(both, None), P(both, None), P(), P(), P(None, both), P(), P("blk"), P("blk"))
    return jax.shard_map(per_device, mesh=mesh, in_specs=placed, out_specs=P("blk", "tp"), check_vma=False)
```

```python
import jax
import jax.numpy as jnp
import numpy as np
from jax import lax
from jax.experimental import pallas as pl
from jax.experimental.pallas import tpu as pltpu
from jax.sharding import PartitionSpec as P

D = 5120
HD = 128
TOK = 512
ROWS = 20
WC = 384
NORM_FLOOR = 0.0625
ROPE_BASE = 1000000.0
NEGATIVE_FILL = -1e30
LOG2E = 1.4426950408889634
MESH = pl.DeviceIdType.MESH
VM = pltpu.VMEM
DMA = pltpu.SemaphoreType.DMA
BF = jnp.bfloat16
F32 = jnp.float32
VLIM = 62 * 1024 * 1024
PIO2 = (1.5703125, 4.83751296997e-04, 7.54978995489e-08)


def coords():
    b = lax.axis_index("blk")
    t = lax.axis_index("tp")
    return b, t, b // 4, (b // 2) % 2, b % 2, t // 4, t % 4


def blk_of(x, zl, c):
    return x * 4 + zl * 2 + c


def signal(dev):
    pl.semaphore_signal(pltpu.get_barrier_semaphore(), inc=1, device_id=dev, device_id_type=MESH)


def push(src, dst, ssem, rsem, dev):
    pltpu.make_async_remote_copy(src, dst, ssem, rsem, device_id=dev, device_id_type=MESH).start()


def landed(ref, sem):
    pltpu.make_async_copy(ref, ref, sem).wait()


def sends_of(pieces):
    return 15 * pieces


class Gather:
    def __init__(self, at, pieces, send, recv):
        self.at, self.n, self.send, self.recv = at, pieces, send, recv
        b, t, x, zl, c, y, zh = coords()
        self.t = t
        self.own = b
        self.sib = blk_of(x, zl, 1 - c)
        self.z = blk_of(x, 1 - zl, c)
        xp, xm, x2 = (x + 1) % 4, (x + 3) % 4, (x + 2) % 4
        self.xp, self.xm = blk_of(xp, zl, c), blk_of(xm, zl, c)
        self.xpz, self.xmz = blk_of(xp, 1 - zl, c), blk_of(xm, 1 - zl, c)
        self.x2, self.x2z = blk_of(x2, zl, c), blk_of(x2, 1 - zl, c)
        self.order = (self.own, self.z, self.xm, self.xp, self.xmz, self.xpz, self.x2, self.x2z)
        self.count = 0
        self.sent = []

    def _send(self, chunk, p, to):
        ref = self.at(chunk, p)
        k = self.count
        self.count += 1
        push(ref, ref, self.send.at[k], self.recv.at[chunk, p], {"blk": to, "tp": self.t})
        self.sent.append((p, k))

    def wait(self, chunk, p):
        landed(self.at(chunk, p), self.recv.at[chunk, p])

    def mine(self, *pieces):
        for p in pieces:
            for to in (self.xp, self.xm, self.z, self.sib):
                self._send(self.own, p, to)

    def zfwd(self, *pieces):
        for p in pieces:
            self.wait(self.z, p)
            for to in (self.xp, self.xm, self.sib):
                self._send(self.z, p, to)

    def side(self, zside, *pieces):
        minus, plus = (self.xmz, self.xpz) if zside else (self.xm, self.xp)
        for p in pieces:
            self.wait(minus, p)
            if p % 2 == 0:
                self._send(minus, p, self.xp)
            self._send(minus, p, self.sib)
            self.wait(plus, p)
            if p % 2 == 1:
                self._send(plus, p, self.xm)
            self._send(plus, p, self.sib)

    def far(self, zside, *pieces):
        chunk = self.x2z if zside else self.x2
        for p in pieces:
            self.wait(chunk, p)
            self._send(chunk, p, self.sib)

    def sibs(self, k):
        chunk = flip(self.order[k])
        for p in range(self.n):
            self.wait(chunk, p)

    def drain(self):
        for p, k in self.sent:
            landed(self.at(0, p), self.send.at[k])


def flip(k):
    return k + 1 - 2 * (k % 2)


def pick(options, i):
    r = options[0]
    for k in range(1, len(options)):
        r = jnp.where(i == k, options[k], r)
    return r


def run(n, compute, events):
    def body(i, carry):
        for k, event in events.items():
            pl.when(i == k)(event)
        compute(i)
        return carry

    lax.fori_loop(0, n, body, 0)


def seq(*calls):
    def go():
        for f, *args in calls:
            f(*args)

    return go


def cos_sin(angle):
    k = jnp.floor(angle * (2.0 / np.pi) + 0.5)
    r = ((angle - k * PIO2[0]) - k * PIO2[1]) - k * PIO2[2]
    s = r * r
    sin = r + r * s * (-1.6666654611e-1 + s * (8.3321608736e-3 + s * -1.9515295891e-4))
    cos = 1.0 - 0.5 * s + s * s * (4.166664568298827e-2 + s * (-1.388731625493765e-3 + s * 2.443315711809948e-5))
    m = k.astype(jnp.int32)
    odd = m % 2 == 1
    cos_v = jnp.where(odd, sin, cos)
    sin_v = jnp.where(odd, cos, sin)
    cos_v = jnp.where((m + 1) // 2 % 2 == 1, -cos_v, cos_v)
    sin_v = jnp.where(m // 2 % 2 == 1, -sin_v, sin_v)
    return cos_v, sin_v


def layer(
    dm, x_hbm, wq, wkv, wo, vec, pos, seg, freq,
    out,
    xv, slot, five, ordered, land, wide, w, land_o, wide_o, wog, segs, kaug, acc_w, trig, res, q, kvg, m_s, acc_s, cg, far_b, plus, minus,
    r_far, r_plus, r_minus,
    a_send, a_recv, o_send, o_recv, s_send, s_recv, g_send, g_recv, h_send, h_recv, k_send, k_recv, e_send, c_send, c_recv, p_send, p_recv,
    x_sem,
):
    b, t, x, zl, c, y, zh = coords()
    hl = t % 2
    main = Gather(lambda k, p: w.at[k, pl.ds(p * 80, 80)], 4, g_send, g_recv)
    outw = Gather(lambda k, p: wog.at[k, :, pl.ds(p * 512, 512)], 2, h_send, h_recv)

    def kv_at(k, p):
        lane = pl.multiple_of(128 * ((hl + p // 2) % 2), 128)
        return kvg.at[k, pl.ds(256 * (p % 2), 256), pl.ds(lane, 128)]

    keys = Gather(kv_at, 4, k_send, k_recv)
    tgt_blk = blk_of(x, y // 2, y % 2)
    tgt_tp = [yb * 4 + 2 * zl + c for yb in range(4)]
    src_blk = blk_of(x, zh // 2, zh % 2)
    src_tp = [(2 * zl + c) * 4 + k for k in range(4)]

    def other(kb, kt):
        return jnp.logical_or(kb != b, kt != t)

    x_copy = pltpu.make_async_copy(x_hbm, xv, x_sem)
    x_copy.start()
    for k in range(1, 16):
        signal({"blk": b, "tp": (t + k) % 16})
        signal({"blk": (b + k) % 16, "tp": t})
    for k in range(4):
        @pl.when(other(tgt_blk, tgt_tp[k]))
        def _():
            signal({"blk": tgt_blk, "tp": tgt_tp[k]})

        @pl.when(other(src_blk, src_tp[k]))
        def _():
            signal({"blk": src_blk, "tp": src_tp[k]})
    loop = jnp.logical_and(y == 2 * zl + c, zh == 2 * zl + c).astype(jnp.int32)
    pl.semaphore_wait(pltpu.get_barrier_semaphore(), 38 - 2 * loop)

    def q_src(to):
        return wq.at[:, pl.ds(pl.multiple_of(to * 256, 256), 256)]

    def kv_src(to):
        return wkv.at[:, pl.ds(pl.multiple_of(to * 128, 128), 128)]

    def q_land(k):
        return land.at[k, :, pl.ds(0, 256)]

    def kv_land(k):
        return land.at[k, :, pl.ds(256, 128)]

    for k in (4, 12, 1, 3, 5, 7, 13, 15, 8, 2, 9, 6, 14, 10, 11):
        to = (t + k) % 16
        push(q_src(to), q_land(t), a_send.at[0, k], a_recv.at[0, t], {"blk": b, "tp": to})
        push(kv_src(to), kv_land(t), a_send.at[1, k], a_recv.at[1, t], {"blk": b, "tp": to})
    pltpu.make_async_copy(q_src(t), q_land(t), a_recv.at[0, t]).start()
    pltpu.make_async_copy(kv_src(t), kv_land(t), a_recv.at[1, t]).start()
    for k in range(1, 16):
        push(seg, segs.at[b], s_send.at[k], s_recv.at[b], {"blk": (b + k) % 16, "tp": t})
    segs[b] = seg[...]

    x_copy.wait()

    def squares(j, acc):
        v = xv[:, pl.ds(pl.multiple_of(j * 128, 128), 128)].astype(F32)
        return acc + v * v

    total = lax.fori_loop(0, D // 128, squares, jnp.zeros((TOK, 128), F32))
    square = jnp.maximum(jnp.sum(total, axis=1, keepdims=True) * (1.0 / D), NORM_FLOOR)
    trig[0] = jnp.broadcast_to(lax.rsqrt(square), (TOK, 128))

    def turn(i, carry):
        for k in range(5):
            at = pl.ds(pl.multiple_of(i * 640 + k * 128, 128), 128)
            v = xv[:, at].astype(F32) * trig[0] * vec[:, at]
            five[k * 128 : (k + 1) * 128, :] = v.astype(BF).astype(F32).T
        for k in range(32):
            slot[i * 32 + k] = five[k * ROWS : (k + 1) * ROWS, :]
        return carry

    lax.fori_loop(0, 8, turn, 0)

    def back(i):
        for k in range(32):
            five[k * ROWS : (k + 1) * ROWS, :] = slot[dm[i * 32 + k]]
        for k in range(5):
            at = pl.ds(pl.multiple_of(i * 640 + k * 128, 128), 128)
            ordered[:, at] = five[k * 128 : (k + 1) * 128, :].T.astype(BF)

    def group(g):
        for k in range(4):
            landed(q_land(4 * g + k), a_recv.at[0, 4 * g + k])
            landed(kv_land(4 * g + k), a_recv.at[1, 4 * g + k])
            wide[k * ROWS : (k + 1) * ROWS, :] = land[4 * g + k].astype(F32)
        w[b, pl.ds(g * 80, 80), :] = wide[...].astype(BF)
        main.mine(g)

    def send_out():
        for k in range(4):
            src = wo.at[:, pl.ds(k * 1024, 1024)]

            @pl.when(other(tgt_blk, tgt_tp[k]))
            def _():
                push(src, land_o.at[zh], o_send.at[k], o_recv.at[zh], {"blk": tgt_blk, "tp": tgt_tp[k]})

            @pl.when(jnp.logical_not(other(tgt_blk, tgt_tp[k])))
            def _():
                pltpu.make_async_copy(src, land_o.at[zh], o_recv.at[zh]).start()

    run(8, back, {
        0: seq((group, 0)),
        1: seq((group, 1)),
        2: seq((group, 2), (main.zfwd, 0)),
        3: seq((group, 3), (main.zfwd, 1)),
        4: seq((send_out,), (main.zfwd, 2), (main.side, False, 0)),
        5: seq((main.zfwd, 3), (main.side, False, 1)),
        6: seq((main.side, False, 2)),
        7: seq((main.side, False, 3)),
    })

    angle = freq[...] * pos[...].astype(F32)
    cos_t, sin_t = cos_sin(angle)
    trig[0] = jnp.concatenate([cos_t, cos_t], axis=0).T
    trig[1] = jnp.concatenate([-sin_t, sin_t], axis=0).T
    window = pl.ds(pl.multiple_of(128 * ((5 * t) // 2), 128), 384)
    res[...] = xv[:, window].astype(F32).T

    acc_w[...] = jnp.zeros((TOK, WC), F32)
    row0 = lax.broadcasted_iota(jnp.int32, (HD, TOK), 0) == 0

    def mul(i):
        pair = pick(main.order, i) // 2
        lanes = pl.ds(pl.multiple_of(pair * 640, 640), 640)
        acc_w[...] += jnp.dot(
            ordered[:, lanes], w[pl.ds(pair * 2, 2)].reshape(640, WC), preferred_element_type=F32
        )
        for k in range(2):
            j = 2 * i + k

            @pl.when(j != b)
            def _():
                landed(segs.at[j], s_recv.at[j])

            row = jnp.where(segs[j] == 0, NEGATIVE_FILL, 0.0)
            kaug[j] = jnp.where(row0, jnp.broadcast_to(row, (HD, TOK)), 0.0).T.astype(BF)

    run(8, mul, {
        0: seq((main.side, True, 0, 1), (main.sibs, 0)),
        1: seq((main.side, True, 2, 3), (main.sibs, 1)),
        2: seq((main.far, False, 0, 1), (main.sibs, 2)),
        3: seq((main.far, False, 2, 3), (main.sibs, 3)),
        4: seq((main.sibs, 4),),
        5: seq((main.far, True, 0, 1), (main.sibs, 5)),
        6: seq((main.far, True, 2, 3), (main.sibs, 6)),
        7: seq((main.sibs, 7),),
    })

    is_key = hl == 0
    kv_bias = vec[:, pl.ds(pl.multiple_of(D + 4096 + t * 128, 128), 128)]
    u = acc_w[:, 256:384] + kv_bias
    turned = u * trig[0] + pltpu.roll(u, HD // 2, 1) * trig[1]
    mine = pl.ds(pl.multiple_of(hl * 128, 128), 128)
    kvg[b, :, mine] = jnp.where(is_key, turned, u).astype(BF)
    partner = {"blk": b, "tp": t + 1 - 2 * hl}
    for r in range(2):
        push(kv_at(b, r), kv_at(b, r), e_send.at[r], k_recv.at[b, 2 + r], partner)
        keys.mine(r)
    own_seg = jnp.where(row0, jnp.broadcast_to(seg[...].astype(F32), (HD, TOK)), 0.0).T.astype(BF)
    for h in range(2):
        q_bias = vec[:, pl.ds(pl.multiple_of(D + t * 256 + h * 128, 128), 128)]
        u = acc_w[:, h * HD : (h + 1) * HD] + q_bias
        q[h, :, 0:HD] = (u * trig[0] + pltpu.roll(u, HD // 2, 1) * trig[1]).astype(BF)
        q[h, :, HD:] = own_seg

    coef = HD ** -0.5 * LOG2E
    half = TOK // 2

    def block(j, diagonal):
        kop = jnp.concatenate([kvg[j, :, 0:HD], kaug[j]], axis=1)
        vop = jnp.concatenate([kvg[j, :, HD:], jnp.ones((TOK, HD), BF)], axis=1)
        for h in range(2):
            for r in range(2):
                rows = pl.ds(r * half, half)
                s = lax.dot_general(q[h, rows, :], kop, (((1,), (1,)), ((), ())), preferred_element_type=F32)
                if diagonal:
                    qi = lax.broadcasted_iota(jnp.int32, s.shape, 0) + r * half
                    ki = lax.broadcasted_iota(jnp.int32, s.shape, 1)
                    s = jnp.where(ki <= qi, s, NEGATIVE_FILL)
                peak = jnp.max(s, axis=1, keepdims=True)
                if diagonal:
                    new = peak
                else:
                    old = m_s[h, rows, :]
                    new = jnp.maximum(old, peak)
                    factor = jnp.exp2((old - new) * coef)
                e = jnp.exp2(s * coef - (new * coef)[:, 0:1]).astype(BF)
                o = jnp.dot(e, vop, preferred_element_type=F32)
                if diagonal:
                    m_s[h, rows, :] = jnp.broadcast_to(new, (half, HD))
                    acc_s[h, rows, :] = o
                else:
                    m_s[h, rows, :] = new
                    acc_s[h, rows, 0:HD] = acc_s[h, rows, 0:HD] * factor + o[:, 0:HD]
                    acc_s[h, rows, HD:] = acc_s[h, rows, HD:] * factor + o[:, HD:]

    def squeeze_out():
        for k in range(4):
            landed(land_o.at[k], o_recv.at[k])
            wide_o[k * ROWS : (k + 1) * ROWS, :] = land_o[k].astype(F32)
        wog[b] = wide_o[...].astype(BF)

    keys.zfwd(0, 1)
    keys.side(False, 0, 1)
    for r in range(2):
        keys.wait(b, 2 + r)
        keys.mine(2 + r)
    squeeze_out()
    block(b, True)
    keys.zfwd(2, 3)

    def visit(i):
        chunk = pick(keys.order, i // 2)
        chunk = jnp.where(i % 2 == 1, flip(chunk), chunk)

        @pl.when(chunk < b)
        def _():
            block(chunk, False)

    run(16, visit, {
        0: seq((keys.side, False, 2, 3)),
        1: seq((keys.side, True, 0, 1), (keys.sibs, 0)),
        3: seq((keys.sibs, 1),),
        4: seq((keys.side, True, 2, 3)),
        5: seq((keys.sibs, 2),),
        6: seq((keys.far, False, 0, 1)),
        7: seq((keys.sibs, 3),),
        8: seq((outw.mine, 0, 1)),
        9: seq((keys.far, False, 2, 3), (keys.sibs, 4)),
        10: seq((keys.far, True, 0, 1)),
        11: seq((keys.sibs, 5), (outw.zfwd, 0, 1)),
        12: seq((keys.far, True, 2, 3)),
        13: seq((keys.sibs, 6), (outw.side, False, 0, 1)),
        14: seq((outw.side, True, 0, 1)),
        15: seq((keys.sibs, 7),),
    })

    up, down, opp = (zh + 1) % 4, (zh + 3) % 4, (zh + 2) % 4
    yp, ym, y2 = (y + 1) % 4, (y + 3) % 4, (y + 2) % 4
    zdev = lambda k: {"blk": b, "tp": y * 4 + k}
    ydev = lambda k: {"blk": b, "tp": k * 4 + zh}
    at = lambda k, p: cg.at[k, pl.ds(p * 128, 128)]

    def waitc(k, p):
        landed(at(k, p), c_recv.at[k, p])

    for r in range(2):
        rows = pl.ds(r * half, half)
        for h in range(2):
            cg[zh, rows, h * HD : (h + 1) * HD] = (acc_s[h, rows, 0:HD] / acc_s[h, rows, HD:]).astype(BF)
        for p in (2 * r, 2 * r + 1):
            push(at(zh, p), at(zh, p), c_send.at[0, p], c_recv.at[zh, p], zdev(up))
            push(at(zh, p), at(zh, p), c_send.at[1, p], c_recv.at[zh, p], zdev(down))
        if r == 0:
            outw.far(False, 0, 1)
        waitc(down, 2 * r)
        push(at(down, 2 * r), at(down, 2 * r), c_send.at[2, 2 * r], c_recv.at[down, 2 * r], zdev(up))
        waitc(up, 2 * r + 1)
        push(at(up, 2 * r + 1), at(up, 2 * r + 1), c_send.at[2, 2 * r + 1], c_recv.at[up, 2 * r + 1], zdev(down))
    outw.far(True, 0, 1)
    for k in range(8):
        outw.sibs(k)

    def partial(k, r):
        v = jnp.zeros((320, half), F32)
        for i in range(4):
            v = v + lax.dot_general(
                wog[pl.ds(k * 4, 4), :, i * 256 : (i + 1) * 256].reshape(320, 256),
                cg[i, pl.ds(r * half, half), :],
                (((1,), (1,)), ((), ())),
                preferred_element_type=F32,
            )
        return v

    lo, hi = pl.ds(0, 160), pl.ds(160, 160)
    for r in range(2):
        waitc(down, 2 * r + 1)
        waitc(up, 2 * r)
        waitc(opp, 2 * r)
        waitc(opp, 2 * r + 1)
        far_b[r] = partial(y2, r).astype(BF)
        push(far_b.at[r, lo], r_far.at[r, lo], p_send.at[r, 0], p_recv.at[r, 0], ydev(yp))
        push(far_b.at[r, hi], r_far.at[r, hi], p_send.at[r, 1], p_recv.at[r, 1], ydev(ym))
        v = partial(yp, r)
        plus[r, hi, :] = v[160:].astype(BF)
        push(plus.at[r, hi], r_plus.at[r, hi], p_send.at[r, 2], p_recv.at[r, 2], ydev(yp))
        u = partial(ym, r)
        minus[r, lo, :] = u[:160].astype(BF)
        push(minus.at[r, lo], r_minus.at[r, lo], p_send.at[r, 3], p_recv.at[r, 3], ydev(ym))
        landed(r_far.at[r, lo], p_recv.at[r, 0])
        plus[r, lo, :] = (v[:160] + r_far[r, lo, :].astype(F32)).astype(BF)
        push(plus.at[r, lo], r_plus.at[r, lo], p_send.at[r, 4], p_recv.at[r, 4], ydev(yp))
        landed(r_far.at[r, hi], p_recv.at[r, 1])
        minus[r, hi, :] = (u[160:] + r_far[r, hi, :].astype(F32)).astype(BF)
        push(minus.at[r, hi], r_minus.at[r, hi], p_send.at[r, 5], p_recv.at[r, 5], ydev(ym))
        cols = pl.ds(r * half, half)
        res[pl.ds(0, 320), cols] = partial(y, r) + res[pl.ds(pl.multiple_of(64 * hl, 64), 320), cols]
    for r in range(2):
        for sl, k1, k2 in ((hi, 2, 5), (lo, 4, 3)):
            landed(r_plus.at[r, sl], p_recv.at[r, k1])
            landed(r_minus.at[r, sl], p_recv.at[r, k2])
        cols = pl.ds(r * half, half)
        out[:, cols] = (res[pl.ds(0, 320), cols] + r_plus[r].astype(F32) + r_minus[r].astype(F32)).astype(BF)

    for k in range(1, 16):
        landed(q_land(0), a_send.at[0, k])
        landed(kv_land(0), a_send.at[1, k])
        landed(segs.at[0], s_send.at[k])
    for k in range(4):
        @pl.when(other(tgt_blk, tgt_tp[k]))
        def _():
            landed(land_o.at[k], o_send.at[k])

        landed(at(0, 0), c_send.at[0, k])
        landed(at(0, 0), c_send.at[1, k])
        landed(at(0, 0), c_send.at[2, k])
    for r in range(2):
        landed(kv_at(0, r), e_send.at[r])
        for k in range(6):
            landed(far_b.at[0, lo], p_send.at[r, k])
    main.drain()
    outw.drain()
    keys.drain()


def per_device(residual_in, norm_gain, w_query, w_key_value, query_bias, key_value_bias, w_output, device_map, positions, segments):
    vec = jnp.concatenate([norm_gain, query_bias, key_value_bias]).astype(F32)[None, :]
    freq = (np.float64(ROPE_BASE) ** (-np.arange(HD // 2) * 2.0 / HD)).astype(np.float32)[:, None]
    freq = jnp.asarray(np.repeat(freq, TOK, axis=1))
    hbm = pl.BlockSpec(memory_space=pl.ANY)
    vm = pl.BlockSpec(memory_space=VM)
    turned = pl.pallas_call(
        layer,
        out_shape=jax.ShapeDtypeStruct((320, TOK), BF),
        in_specs=[pl.BlockSpec(memory_space=pltpu.SMEM), hbm, hbm, hbm, hbm, vm, vm, vm, vm],
        out_specs=vm,
        scratch_shapes=[
            VM((TOK, D), BF),
            VM((256, ROWS, TOK), F32),
            VM((640, TOK), F32),
            VM((TOK, D), BF),
            VM((16, ROWS, WC), BF),
            VM((80, WC), F32),
            VM((16, 320, WC), BF),
            VM((4, ROWS, 1024), BF),
            VM((80, 1024), F32),
            VM((16, 80, 1024), BF),
            VM((16, 1, TOK), jnp.int32),
            VM((16, TOK, HD), BF),
            VM((TOK, WC), F32),
            VM((2, TOK, HD), F32),
            VM((384, TOK), F32),
            VM((2, TOK, 256), BF),
            VM((16, TOK, 256), BF),
            VM((2, TOK, HD), F32),
            VM((2, TOK, 256), F32),
            VM((4, TOK, 256), BF),
        ]
        + [VM((2, 320, 256), BF)] * 6
        + [
            DMA((2, 16)), DMA((2, 16)), DMA((4,)), DMA((4,)), DMA((16,)), DMA((16,)),
            DMA((sends_of(4),)), DMA((16, 4)), DMA((sends_of(2),)), DMA((16, 2)), DMA((sends_of(4),)), DMA((16, 4)), DMA((2,)),
            DMA((3, 4)), DMA((4, 4)), DMA((2, 6)), DMA((2, 6)), DMA,
        ],
        compiler_params=pltpu.CompilerParams(collective_id=0, has_side_effects=True, vmem_limit_bytes=VLIM),
        name="layer",
    )(
        device_map, residual_in, w_query, w_key_value, w_output.T, vec,
        positions[None, :], segments[None, :], freq,
    )
    return turned.T


def solution(mesh):
    both = ("blk", "tp")
    placed = (P("blk", None), P(), P(both, None), P(both, None), P(), P(), P(None, both), P(), P("blk"), P("blk"))
    return jax.shard_map(per_device, mesh=mesh, in_specs=placed, out_specs=P("blk", "tp"), check_vma=False)
```

```python
import jax
import jax.numpy as jnp
import numpy as np
from jax import lax
from jax.experimental import pallas as pl
from jax.experimental.pallas import tpu as pltpu
from jax.sharding import PartitionSpec as P

D = 5120
HD = 128
TOK = 512
ROWS = 20
WC = 384
NORM_FLOOR = 0.0625
ROPE_BASE = 1000000.0
NEGATIVE_FILL = -1e30
LOG2E = 1.4426950408889634
MESH = pl.DeviceIdType.MESH
VM = pltpu.VMEM
DMA = pltpu.SemaphoreType.DMA
BF = jnp.bfloat16
F32 = jnp.float32
VLIM = 62 * 1024 * 1024
PIO2 = (1.5703125, 4.83751296997e-04, 7.54978995489e-08)


def coords():
    b = lax.axis_index("blk")
    t = lax.axis_index("tp")
    return b, t, b // 4, (b // 2) % 2, b % 2, t // 4, t % 4


def blk_of(x, zl, c):
    return x * 4 + zl * 2 + c


def signal(dev):
    pl.semaphore_signal(pltpu.get_barrier_semaphore(), inc=1, device_id=dev, device_id_type=MESH)


def push(src, dst, ssem, rsem, dev):
    pltpu.make_async_remote_copy(src, dst, ssem, rsem, device_id=dev, device_id_type=MESH).start()


def landed(ref, sem):
    pltpu.make_async_copy(ref, ref, sem).wait()


def sends_of(pieces):
    return 15 * pieces


class Gather:
    def __init__(self, at, pieces, send, recv):
        self.at, self.n, self.send, self.recv = at, pieces, send, recv
        b, t, x, zl, c, y, zh = coords()
        self.t = t
        self.own = b
        self.sib = blk_of(x, zl, 1 - c)
        self.z = blk_of(x, 1 - zl, c)
        xp, xm, x2 = (x + 1) % 4, (x + 3) % 4, (x + 2) % 4
        self.xp, self.xm = blk_of(xp, zl, c), blk_of(xm, zl, c)
        self.xpz, self.xmz = blk_of(xp, 1 - zl, c), blk_of(xm, 1 - zl, c)
        self.x2, self.x2z = blk_of(x2, zl, c), blk_of(x2, 1 - zl, c)
        self.order = (self.own, self.z, self.xm, self.xp, self.xmz, self.xpz, self.x2, self.x2z)
        self.count = 0
        self.sent = []

    def _send(self, chunk, p, to):
        ref = self.at(chunk, p)
        k = self.count
        self.count += 1
        push(ref, ref, self.send.at[k], self.recv.at[chunk, p], {"blk": to, "tp": self.t})
        self.sent.append((p, k))

    def wait(self, chunk, p):
        landed(self.at(chunk, p), self.recv.at[chunk, p])

    def mine(self, *pieces):
        for p in pieces:
            for to in (self.xp, self.xm, self.z, self.sib):
                self._send(self.own, p, to)

    def zfwd(self, *pieces):
        for p in pieces:
            self.wait(self.z, p)
            for to in (self.xp, self.xm, self.sib):
                self._send(self.z, p, to)

    def side(self, zside, *pieces):
        minus, plus = (self.xmz, self.xpz) if zside else (self.xm, self.xp)
        for p in pieces:
            self.wait(minus, p)
            if p % 2 == 0:
                self._send(minus, p, self.xp)
            self._send(minus, p, self.sib)
            self.wait(plus, p)
            if p % 2 == 1:
                self._send(plus, p, self.xm)
            self._send(plus, p, self.sib)

    def far(self, zside, *pieces):
        chunk = self.x2z if zside else self.x2
        for p in pieces:
            self.wait(chunk, p)
            self._send(chunk, p, self.sib)

    def sibs(self, k):
        chunk = flip(self.order[k])
        for p in range(self.n):
            self.wait(chunk, p)

    def drain(self):
        for p, k in self.sent:
            landed(self.at(0, p), self.send.at[k])


def flip(k):
    return k + 1 - 2 * (k % 2)


def pick(options, i):
    r = options[0]
    for k in range(1, len(options)):
        r = jnp.where(i == k, options[k], r)
    return r


def run(n, compute, events):
    def body(i, carry):
        for k, event in events.items():
            pl.when(i == k)(event)
        compute(i)
        return carry

    lax.fori_loop(0, n, body, 0)


def seq(*calls):
    def go():
        for f, *args in calls:
            f(*args)

    return go


def cos_sin(angle):
    k = jnp.floor(angle * (2.0 / np.pi) + 0.5)
    r = ((angle - k * PIO2[0]) - k * PIO2[1]) - k * PIO2[2]
    s = r * r
    sin = r + r * s * (-1.6666654611e-1 + s * (8.3321608736e-3 + s * -1.9515295891e-4))
    cos = 1.0 - 0.5 * s + s * s * (4.166664568298827e-2 + s * (-1.388731625493765e-3 + s * 2.443315711809948e-5))
    m = k.astype(jnp.int32)
    odd = m % 2 == 1
    cos_v = jnp.where(odd, sin, cos)
    sin_v = jnp.where(odd, cos, sin)
    cos_v = jnp.where((m + 1) // 2 % 2 == 1, -cos_v, cos_v)
    sin_v = jnp.where(m // 2 % 2 == 1, -sin_v, sin_v)
    return cos_v, sin_v


def layer(
    dm, x_hbm, wq, wkv, wo, gain_h, qb_h, kb_h, pos_h, seg_h, freq_h,
    out,
    xv, slot, five, ordered, land, wide, w, land_o, wide_o, wog, segs, kaug, acc_w, trig, res, q, kvg, m_s, acc_s, cg, far_b, plus, minus,
    r_far, r_plus, r_minus,
    a_send, a_recv, o_send, o_recv, s_send, s_recv, g_send, g_recv, h_send, h_recv, k_send, k_recv, e_send, c_send, c_recv, p_send, p_recv,
    x_sem, gain, qb, kb, pos, seg, freq, gain_row, i_sem,
):
    b, t, x, zl, c, y, zh = coords()
    hl = t % 2
    main = Gather(lambda k, p: w.at[k, pl.ds(pl.multiple_of((zh + p) % 4 * 80, 80), 80)], 4, g_send, g_recv)
    outw = Gather(lambda k, p: wog.at[k, :, pl.ds(p * 512, 512)], 2, h_send, h_recv)

    def kv_at(k, p):
        lane = pl.multiple_of(128 * ((hl + p // 2) % 2), 128)
        return kvg.at[k, pl.ds(256 * (p % 2), 256), pl.ds(lane, 128)]

    keys = Gather(kv_at, 4, k_send, k_recv)
    tgt_blk = blk_of(x, y // 2, y % 2)
    tgt_tp = [yb * 4 + 2 * zl + c for yb in range(4)]
    src_blk = blk_of(x, zh // 2, zh % 2)
    src_tp = [(2 * zl + c) * 4 + k for k in range(4)]

    def other(kb, kt):
        return jnp.logical_or(kb != b, kt != t)

    x_copy = pltpu.make_async_copy(x_hbm, xv, x_sem)
    x_copy.start()
    in_copy = [
        pltpu.make_async_copy(src, dst, i_sem.at[k])
        for k, (src, dst) in enumerate(((gain_h, gain), (qb_h, qb), (kb_h, kb), (pos_h, pos), (seg_h, seg), (freq_h, freq)))
    ]
    for copy in in_copy:
        copy.start()
    for k in range(1, 16):
        signal({"blk": b, "tp": (t + k) % 16})
        signal({"blk": (b + k) % 16, "tp": t})
    for k in range(4):
        @pl.when(other(tgt_blk, tgt_tp[k]))
        def _():
            signal({"blk": tgt_blk, "tp": tgt_tp[k]})

        @pl.when(other(src_blk, src_tp[k]))
        def _():
            signal({"blk": src_blk, "tp": src_tp[k]})
    loop = jnp.logical_and(y == 2 * zl + c, zh == 2 * zl + c).astype(jnp.int32)
    pl.semaphore_wait(pltpu.get_barrier_semaphore(), 38 - 2 * loop)

    def q_src(to):
        return wq.at[:, pl.ds(pl.multiple_of(to * 256, 256), 256)]

    def kv_src(to):
        return wkv.at[:, pl.ds(pl.multiple_of(to * 128, 128), 128)]

    def q_land(k):
        return land.at[k, :, pl.ds(0, 256)]

    def kv_land(k):
        return land.at[k, :, pl.ds(256, 128)]

    for k in range(1, 16):
        to = (y + k) % 4 * 4 + (zh + (0, 3, 1, 2)[k // 4]) % 4
        push(q_src(to), q_land(t), a_send.at[0, k], a_recv.at[0, t], {"blk": b, "tp": to})
        push(kv_src(to), kv_land(t), a_send.at[1, k], a_recv.at[1, t], {"blk": b, "tp": to})
    pltpu.make_async_copy(q_src(t), q_land(t), a_recv.at[0, t]).start()
    pltpu.make_async_copy(kv_src(t), kv_land(t), a_recv.at[1, t]).start()

    def send_segs():
        in_copy[4].wait()
        for k in range(1, 16):
            push(seg, segs.at[b], s_send.at[k], s_recv.at[b], {"blk": (b + k) % 16, "tp": t})
        segs[b] = seg[...]


    in_copy[0].wait()
    for k in range(D // 256):
        gain_row[:, k * 256 : (k + 1) * 256] = gain[k * 256 : (k + 1) * 256].astype(F32)[None, :]
    x_copy.wait()

    def squares(j, acc):
        v = xv[:, pl.ds(pl.multiple_of(j * 128, 128), 128)].astype(F32)
        return acc + v * v

    total = lax.fori_loop(0, D // 128, squares, jnp.zeros((TOK, 128), F32))
    square = jnp.maximum(jnp.sum(total, axis=1, keepdims=True) * (1.0 / D), NORM_FLOOR)
    trig[0] = jnp.broadcast_to(lax.rsqrt(square), (TOK, 128))

    def turn(i, carry):
        for k in range(5):
            at = pl.ds(pl.multiple_of(i * 640 + k * 128, 128), 128)
            v = xv[:, at].astype(F32) * trig[0] * gain_row[:, at]
            five[k * 128 : (k + 1) * 128, :] = v.astype(BF).astype(F32).T
        for k in range(32):
            slot[i * 32 + k] = five[k * ROWS : (k + 1) * ROWS, :]
        return carry

    lax.fori_loop(0, 8, turn, 0)

    def back(i):
        for k in range(32):
            f = k // 16 * 16 + k % 4 * 4 + k // 4 % 4
            five[k * ROWS : (k + 1) * ROWS, :] = slot[dm[i * 32 + f]]
        for k in range(5):
            at = pl.ds(pl.multiple_of(i * 640 + k * 128, 128), 128)
            ordered[:, at] = five[k * 128 : (k + 1) * 128, :].T.astype(BF)

    def group(g):
        zs = (zh + g) % 4
        for k in range(4):
            frm = 4 * k + zs
            landed(q_land(frm), a_recv.at[0, frm])
            landed(kv_land(frm), a_recv.at[1, frm])
            wide[k * ROWS : (k + 1) * ROWS, :] = land[frm].astype(F32)
        w[b, pl.ds(pl.multiple_of(zs * 80, 80), 80), :] = wide[...].astype(BF)
        main.mine(g)

    def send_out():
        for k in range(4):
            src = wo.at[:, pl.ds(k * 1024, 1024)]

            @pl.when(other(tgt_blk, tgt_tp[k]))
            def _():
                push(src, land_o.at[zh], o_send.at[k], o_recv.at[zh], {"blk": tgt_blk, "tp": tgt_tp[k]})

            @pl.when(jnp.logical_not(other(tgt_blk, tgt_tp[k])))
            def _():
                pltpu.make_async_copy(src, land_o.at[zh], o_recv.at[zh]).start()

    group(0)
    run(8, back, {
        0: seq((group, 1)),
        1: seq((group, 3), (main.zfwd, 0)),
        2: seq((group, 2), (main.side, False, 0)),
        3: seq((send_segs,), (send_out,), (main.zfwd, 1)),
        4: seq((main.zfwd, 3), (main.side, False, 1)),
        5: seq((main.zfwd, 2), (main.side, True, 0)),
        6: seq((main.side, False, 3)),
        7: seq((main.side, False, 2)),
    })

    for k in (1, 2, 3, 5):
        in_copy[k].wait()
    angle = freq[...] * pos[...].astype(F32)
    cos_t, sin_t = cos_sin(angle)
    trig[0] = jnp.concatenate([cos_t, cos_t], axis=0).T
    trig[1] = jnp.concatenate([-sin_t, sin_t], axis=0).T
    window = pl.ds(pl.multiple_of(128 * ((5 * t) // 2), 128), 384)
    res[...] = xv[:, window].astype(F32).T

    acc_w[...] = jnp.zeros((TOK, WC), F32)
    row0 = lax.broadcasted_iota(jnp.int32, (HD, TOK), 0) == 0

    def mul(i):
        pair = pick(main.order, i) // 2
        lanes = pl.ds(pl.multiple_of(pair * 640, 640), 640)
        acc_w[...] += jnp.dot(
            ordered[:, lanes], w[pl.ds(pair * 2, 2)].reshape(640, WC), preferred_element_type=F32
        )
        for k in range(2):
            j = 2 * i + k

            @pl.when(j != b)
            def _():
                landed(segs.at[j], s_recv.at[j])

            row = jnp.where(segs[j] == 0, NEGATIVE_FILL, 0.0)
            kaug[j] = jnp.where(row0, jnp.broadcast_to(row, (HD, TOK)), 0.0).T.astype(BF)

    run(8, mul, {
        0: seq((main.far, False, 0), (main.side, True, 1), (main.sibs, 0)),
        1: seq((main.far, False, 1), (main.side, True, 3), (main.sibs, 1)),
        2: seq((main.side, True, 2), (main.far, False, 3), (main.sibs, 2)),
        3: seq((main.far, False, 2), (main.far, True, 0), (main.sibs, 3)),
        4: seq((main.far, True, 1), (main.sibs, 4)),
        5: seq((main.far, True, 3), (main.sibs, 5)),
        6: seq((main.far, True, 2), (main.sibs, 6)),
        7: seq((main.sibs, 7),),
    })

    is_key = hl == 0
    kv_pair = kb[pl.ds(pl.multiple_of(t // 2 * 256, 256), 256)].astype(F32)[None, :]
    kv_bias = jnp.where(is_key, kv_pair[:, :HD], kv_pair[:, HD:])
    q_bias = qb[pl.ds(pl.multiple_of(t * 256, 256), 256)].astype(F32)[None, :]
    u = acc_w[:, 256:384] + kv_bias
    turned = u * trig[0] + pltpu.roll(u, HD // 2, 1) * trig[1]
    mine = pl.ds(pl.multiple_of(hl * 128, 128), 128)
    kvg[b, :, mine] = jnp.where(is_key, turned, u).astype(BF)
    partner = {"blk": b, "tp": t + 1 - 2 * hl}
    for r in range(2):
        push(kv_at(b, r), kv_at(b, r), e_send.at[r], k_recv.at[b, 2 + r], partner)
        keys.mine(r)
    own_seg = jnp.where(row0, jnp.broadcast_to(seg[...].astype(F32), (HD, TOK)), 0.0).T.astype(BF)
    for h in range(2):
        u = acc_w[:, h * HD : (h + 1) * HD] + q_bias[:, h * HD : (h + 1) * HD]
        u = (u * trig[0] + pltpu.roll(u, HD // 2, 1) * trig[1]).astype(BF)
        for r in range(2):
            q[r, h * 256 : (h + 1) * 256, 0:HD] = u[r * 256 : (r + 1) * 256]
            q[r, h * 256 : (h + 1) * 256, HD:] = own_seg[r * 256 : (r + 1) * 256]

    coef = HD ** -0.5 * LOG2E
    half = TOK // 2

    def block(pair, r, first):
        ss = []
        for k in range(2):
            j = 2 * pair + k
            kop = jnp.concatenate([kvg[j, :, 0:HD], kaug[j]], axis=1)
            v = lax.dot_general(q[r], kop, (((1,), (1,)), ((), ())), preferred_element_type=F32)
            if first:
                qi = lax.broadcasted_iota(jnp.int32, (TOK, TOK), 0) % half + r * half + c * TOK
                ki = lax.broadcasted_iota(jnp.int32, (TOK, TOK), 1) + k * TOK
                v = jnp.where(ki <= qi, v, NEGATIVE_FILL)
            ss += [v[:, i * HD : (i + 1) * HD] for i in range(4)]
        top = ss
        while len(top) > 1:
            top = [jnp.maximum(top[i], top[i + 1]) for i in range(0, len(top), 2)]
        new = jnp.broadcast_to(jnp.max(top[0], axis=1, keepdims=True), (TOK, HD))
        if not first:
            old = m_s[r]
            new = jnp.maximum(old, new)
            factor = jnp.exp2((old - new) * coef)
        o = jnp.zeros((TOK, 2 * HD), F32)
        for k in range(2):
            e = jnp.concatenate([jnp.exp2((ss[4 * k + i] - new) * coef).astype(BF) for i in range(4)], axis=1)
            vop = jnp.concatenate([kvg[2 * pair + k, :, HD:], jnp.ones((TOK, HD), BF)], axis=1)
            o = o + jnp.dot(e, vop, preferred_element_type=F32)
        m_s[r] = new
        if first:
            acc_s[r] = o
        else:
            acc_s[r, :, 0:HD] = acc_s[r, :, 0:HD] * factor + o[:, 0:HD]
            acc_s[r, :, HD:] = acc_s[r, :, HD:] * factor + o[:, HD:]

    def squeeze_out():
        for k in range(4):
            landed(land_o.at[k], o_recv.at[k])
            wide_o[k * ROWS : (k + 1) * ROWS, :] = land_o[k].astype(F32)
        wog[b] = wide_o[...].astype(BF)

    keys.zfwd(0, 1)
    keys.side(False, 0, 1)
    for r in range(2):
        keys.wait(b, 2 + r)
        keys.mine(2 + r)
    squeeze_out()
    keys.sibs(0)
    block(b // 2, 0, True)
    keys.zfwd(2, 3)

    def visit(r):
        def go(i):
            pair = pick(keys.order[1:], i) // 2

            @pl.when(pair < b // 2)
            def _():
                block(pair, r, False)

        return go

    run(7, visit(0), {
        0: seq((keys.side, False, 2, 3), (keys.side, True, 0, 1), (keys.sibs, 1)),
        1: seq((keys.far, False, 0, 1), (keys.sibs, 2)),
        2: seq((keys.side, True, 2, 3), (keys.sibs, 3)),
        3: seq((keys.far, True, 0, 1), (keys.far, False, 2, 3), (keys.sibs, 4)),
        4: seq((keys.sibs, 5),),
        5: seq((keys.far, True, 2, 3), (outw.mine, 0, 1), (keys.sibs, 6)),
        6: seq((keys.sibs, 7),),
    })

    up, down, opp = (zh + 1) % 4, (zh + 3) % 4, (zh + 2) % 4
    yp, ym, y2 = (y + 1) % 4, (y + 3) % 4, (y + 2) % 4
    zdev = lambda k: {"blk": b, "tp": y * 4 + k}
    ydev = lambda k: {"blk": b, "tp": k * 4 + zh}
    at = lambda k, p: cg.at[k, pl.ds(p * 128, 128)]

    def waitc(k, p):
        landed(at(k, p), c_recv.at[k, p])

    def mine_c(r):
        rows = pl.ds(r * half, half)
        for h in range(2):
            hr = pl.ds(h * half, half)
            cg[zh, rows, h * HD : (h + 1) * HD] = (acc_s[r, hr, 0:HD] / acc_s[r, hr, HD:]).astype(BF)
        for p in (2 * r, 2 * r + 1):
            push(at(zh, p), at(zh, p), c_send.at[0, p], c_recv.at[zh, p], zdev(up))
            push(at(zh, p), at(zh, p), c_send.at[1, p], c_recv.at[zh, p], zdev(down))

    def fwd_c(r):
        waitc(down, 2 * r)
        push(at(down, 2 * r), at(down, 2 * r), c_send.at[2, 2 * r], c_recv.at[down, 2 * r], zdev(up))
        waitc(up, 2 * r + 1)
        push(at(up, 2 * r + 1), at(up, 2 * r + 1), c_send.at[2, 2 * r + 1], c_recv.at[up, 2 * r + 1], zdev(down))

    mine_c(0)
    outw.zfwd(0, 1)
    block(b // 2, 1, True)
    run(7, visit(1), {
        1: seq((outw.side, False, 0, 1)),
        3: seq((fwd_c, 0), (outw.side, True, 0, 1)),
        5: seq((outw.far, False, 0, 1)),
        6: seq((outw.far, True, 0, 1)),
    })
    mine_c(1)
    for k in range(8):
        outw.sibs(k)

    def partial(k, r):
        v = jnp.zeros((320, half), F32)
        for i in range(4):
            v = v + lax.dot_general(
                wog[pl.ds(k * 4, 4), :, i * 256 : (i + 1) * 256].reshape(320, 256),
                cg[i, pl.ds(r * half, half), :],
                (((1,), (1,)), ((), ())),
                preferred_element_type=F32,
            )
        return v

    lo, hi = pl.ds(0, 160), pl.ds(160, 160)
    kept = {}

    def scatter_far(r):
        waitc(down, 2 * r + 1)
        waitc(up, 2 * r)
        waitc(opp, 2 * r)
        waitc(opp, 2 * r + 1)
        far_b[r] = partial(y2, r).astype(BF)
        push(far_b.at[r, lo], r_far.at[r, lo], p_send.at[r, 0], p_recv.at[r, 0], ydev(yp))
        push(far_b.at[r, hi], r_far.at[r, hi], p_send.at[r, 1], p_recv.at[r, 1], ydev(ym))
        v = partial(yp, r)
        plus[r, hi, :] = v[160:].astype(BF)
        push(plus.at[r, hi], r_plus.at[r, hi], p_send.at[r, 2], p_recv.at[r, 2], ydev(yp))
        u = partial(ym, r)
        minus[r, lo, :] = u[:160].astype(BF)
        push(minus.at[r, lo], r_minus.at[r, lo], p_send.at[r, 3], p_recv.at[r, 3], ydev(ym))
        kept[r] = v[:160], u[160:]

    def scatter_near(r):
        v, u = kept[r]
        landed(r_far.at[r, lo], p_recv.at[r, 0])
        plus[r, lo, :] = (v + r_far[r, lo, :].astype(F32)).astype(BF)
        push(plus.at[r, lo], r_plus.at[r, lo], p_send.at[r, 4], p_recv.at[r, 4], ydev(yp))
        landed(r_far.at[r, hi], p_recv.at[r, 1])
        minus[r, hi, :] = (u + r_far[r, hi, :].astype(F32)).astype(BF)
        push(minus.at[r, hi], r_minus.at[r, hi], p_send.at[r, 5], p_recv.at[r, 5], ydev(ym))

    def keep(r):
        cols = pl.ds(r * half, half)
        res[pl.ds(0, 320), cols] = partial(y, r) + res[pl.ds(pl.multiple_of(64 * hl, 64), 320), cols]

    def finish(r):
        for sl, k1, k2 in ((hi, 2, 5), (lo, 4, 3)):
            landed(r_plus.at[r, sl], p_recv.at[r, k1])
            landed(r_minus.at[r, sl], p_recv.at[r, k2])
        cols = pl.ds(r * half, half)
        out[:, cols] = (res[pl.ds(0, 320), cols] + r_plus[r].astype(F32) + r_minus[r].astype(F32)).astype(BF)

    scatter_far(0)
    keep(0)
    scatter_near(0)
    fwd_c(1)
    scatter_far(1)
    keep(1)
    scatter_near(1)
    finish(0)
    finish(1)

    for k in range(1, 16):
        landed(q_land(0), a_send.at[0, k])
        landed(kv_land(0), a_send.at[1, k])
        landed(segs.at[0], s_send.at[k])
    for k in range(4):
        @pl.when(other(tgt_blk, tgt_tp[k]))
        def _():
            landed(land_o.at[k], o_send.at[k])

        landed(at(0, 0), c_send.at[0, k])
        landed(at(0, 0), c_send.at[1, k])
        landed(at(0, 0), c_send.at[2, k])
    for r in range(2):
        landed(kv_at(0, r), e_send.at[r])
        for k in range(6):
            landed(far_b.at[0, lo], p_send.at[r, k])
    main.drain()
    outw.drain()
    keys.drain()


def per_device(residual_in, norm_gain, w_query, w_key_value, query_bias, key_value_bias, w_output, device_map, positions, segments):
    freq = (np.float64(ROPE_BASE) ** (-np.arange(HD // 2) * 2.0 / HD)).astype(np.float32)[:, None]
    freq = jnp.asarray(np.repeat(freq, TOK, axis=1))
    hbm = pl.BlockSpec(memory_space=pl.ANY)
    vm = pl.BlockSpec(memory_space=VM)
    turned = pl.pallas_call(
        layer,
        out_shape=jax.ShapeDtypeStruct((320, TOK), BF),
        in_specs=[pl.BlockSpec(memory_space=pltpu.SMEM), hbm, hbm, hbm, hbm, hbm, hbm, hbm, hbm, hbm, hbm],
        out_specs=vm,
        scratch_shapes=[
            VM((TOK, D), BF),
            VM((256, ROWS, TOK), F32),
            VM((640, TOK), F32),
            VM((TOK, D), BF),
            VM((16, ROWS, WC), BF),
            VM((80, WC), F32),
            VM((16, 320, WC), BF),
            VM((4, ROWS, 1024), BF),
            VM((80, 1024), F32),
            VM((16, 80, 1024), BF),
            VM((16, 1, TOK), jnp.int32),
            VM((16, TOK, HD), BF),
            VM((TOK, WC), F32),
            VM((2, TOK, HD), F32),
            VM((384, TOK), F32),
            VM((2, TOK, 256), BF),
            VM((16, TOK, 256), BF),
            VM((2, TOK, HD), F32),
            VM((2, TOK, 256), F32),
            VM((4, TOK, 256), BF),
        ]
        + [VM((2, 320, 256), BF)] * 6
        + [
            DMA((2, 16)), DMA((2, 16)), DMA((4,)), DMA((4,)), DMA((16,)), DMA((16,)),
            DMA((sends_of(4),)), DMA((16, 4)), DMA((sends_of(2),)), DMA((16, 2)), DMA((sends_of(4),)), DMA((16, 4)), DMA((2,)),
            DMA((3, 4)), DMA((4, 4)), DMA((2, 6)), DMA((2, 6)), DMA,
            VM((D,), BF), VM((4096,), BF), VM((2048,), BF), VM((1, TOK), jnp.int32), VM((1, TOK), jnp.int32), VM((HD // 2, TOK), F32), VM((1, D), F32),
            DMA((6,)),
        ],
        compiler_params=pltpu.CompilerParams(collective_id=0, has_side_effects=True, vmem_limit_bytes=VLIM),
        name="layer",
    )(
        device_map, residual_in, w_query, w_key_value, w_output.T, norm_gain, query_bias, key_value_bias,
        positions[None, :], segments[None, :], freq,
    )
    return turned.T


def solution(mesh):
    both = ("blk", "tp")
    placed = (P("blk", None), P(), P(both, None), P(both, None), P(), P(), P(None, both), P(), P("blk"), P("blk"))
    return jax.shard_map(per_device, mesh=mesh, in_specs=placed, out_specs=P("blk", "tp"), check_vma=False)
```

```python
import jax
import jax.numpy as jnp
import numpy as np
from jax import lax
from jax.experimental import pallas as pl
from jax.experimental.pallas import tpu as pltpu
from jax.sharding import PartitionSpec as P

D = 5120
HD = 128
TOK = 512
ROWS = 20
WC = 384
NORM_FLOOR = 0.0625
ROPE_BASE = 1000000.0
NEGATIVE_FILL = -1e30
LOG2E = 1.4426950408889634
MESH = pl.DeviceIdType.MESH
VM = pltpu.VMEM
DMA = pltpu.SemaphoreType.DMA
BF = jnp.bfloat16
F32 = jnp.float32
VLIM = 62 * 1024 * 1024
PIO2 = (1.5703125, 4.83751296997e-04, 7.54978995489e-08)


def coords():
    b = lax.axis_index("blk")
    t = lax.axis_index("tp")
    return b, t, b // 4, (b // 2) % 2, b % 2, t // 4, t % 4


def blk_of(x, zl, c):
    return x * 4 + zl * 2 + c


def signal(dev):
    pl.semaphore_signal(pltpu.get_barrier_semaphore(), inc=1, device_id=dev, device_id_type=MESH)


def push(src, dst, ssem, rsem, dev):
    pltpu.make_async_remote_copy(src, dst, ssem, rsem, device_id=dev, device_id_type=MESH).start()


def landed(ref, sem):
    pltpu.make_async_copy(ref, ref, sem).wait()


def sends_of(pieces):
    return 15 * pieces


class Gather:
    def __init__(self, at, pieces, send, recv, xfirst=()):
        self.at, self.n, self.send, self.recv, self.xfirst = at, pieces, send, recv, xfirst
        b, t, x, zl, c, y, zh = coords()
        self.t = t
        self.own = b
        self.sib = blk_of(x, zl, 1 - c)
        self.z = blk_of(x, 1 - zl, c)
        xp, xm, x2 = (x + 1) % 4, (x + 3) % 4, (x + 2) % 4
        self.xp, self.xm = blk_of(xp, zl, c), blk_of(xm, zl, c)
        self.xpz, self.xmz = blk_of(xp, 1 - zl, c), blk_of(xm, 1 - zl, c)
        self.x2, self.x2z = blk_of(x2, zl, c), blk_of(x2, 1 - zl, c)
        self.order = (self.own, self.z, self.xm, self.xp, self.xmz, self.xpz, self.x2, self.x2z)
        self.count = 0
        self.sent = []

    def _send(self, chunk, p, to):
        ref = self.at(chunk, p)
        k = self.count
        self.count += 1
        push(ref, ref, self.send.at[k], self.recv.at[chunk, p], {"blk": to, "tp": self.t})
        self.sent.append((p, k))

    def wait(self, chunk, p):
        landed(self.at(chunk, p), self.recv.at[chunk, p])

    def own_z(self, *pieces):
        for p in pieces:
            for to in (self.z, self.sib):
                self._send(self.own, p, to)

    def own_x(self, *pieces):
        for p in pieces:
            for to in (self.xp, self.xm):
                self._send(self.own, p, to)

    def mine(self, *pieces):
        for p in pieces:
            self.own_x(p)
            self.own_z(p)

    def z_in(self, *pieces):
        for p in pieces:
            self.wait(self.z, p)
            self._send(self.z, p, self.sib)

    def z_out(self, *pieces):
        for p in pieces:
            for to in (self.xp, self.xm):
                self._send(self.z, p, to)

    def zfwd(self, *pieces):
        for p in pieces:
            self.wait(self.z, p)
            if p not in self.xfirst:
                self.z_out(p)
            self._send(self.z, p, self.sib)

    def side(self, zside, *pieces):
        minus, plus = (self.xmz, self.xpz) if zside else (self.xm, self.xp)
        for p in pieces:
            for chunk, on, even in ((minus, self.xp, 0), (plus, self.xm, 1)):
                self.wait(chunk, p)
                if p % 2 == even and not (zside and p in self.xfirst):
                    self._send(chunk, p, on)
                if p in self.xfirst and not zside:
                    self._send(chunk, p, self.z)
                self._send(chunk, p, self.sib)

    def far(self, zside, *pieces):
        chunk = self.x2z if zside else self.x2
        for p in pieces:
            self.wait(chunk, p)
            if p in self.xfirst and not zside:
                self._send(chunk, p, self.z)
            self._send(chunk, p, self.sib)

    def sibs(self, k):
        chunk = flip(self.order[k])
        for p in range(self.n):
            self.wait(chunk, p)

    def drain(self):
        for p, k in self.sent:
            landed(self.at(0, p), self.send.at[k])


def flip(k):
    return k + 1 - 2 * (k % 2)


def pick(options, i):
    r = options[0]
    for k in range(1, len(options)):
        r = jnp.where(i == k, options[k], r)
    return r


def run(n, compute, events):
    def body(i, carry):
        for k, event in events.items():
            pl.when(i == k)(event)
        compute(i)
        return carry

    lax.fori_loop(0, n, body, 0)


def seq(*calls):
    def go():
        for f, *args in calls:
            f(*args)

    return go


def cos_sin(angle):
    k = jnp.floor(angle * (2.0 / np.pi) + 0.5)
    r = ((angle - k * PIO2[0]) - k * PIO2[1]) - k * PIO2[2]
    s = r * r
    sin = r + r * s * (-1.6666654611e-1 + s * (8.3321608736e-3 + s * -1.9515295891e-4))
    cos = 1.0 - 0.5 * s + s * s * (4.166664568298827e-2 + s * (-1.388731625493765e-3 + s * 2.443315711809948e-5))
    m = k.astype(jnp.int32)
    odd = m % 2 == 1
    cos_v = jnp.where(odd, sin, cos)
    sin_v = jnp.where(odd, cos, sin)
    cos_v = jnp.where((m + 1) // 2 % 2 == 1, -cos_v, cos_v)
    sin_v = jnp.where(m // 2 % 2 == 1, -sin_v, sin_v)
    return cos_v, sin_v


def layer(
    dm, x_hbm, wq, wkv, wo, gain_h, qb_h, kb_h, pos_h, seg_h, freq_h,
    out,
    xv, slot, five, ordered, land, wide, w, land_o, wide_o, wog, segs, kaug, acc_w, trig, res, q, kvg, m_s, acc_s, cg,
    fb0, pb0, mb0, rf0, rp0, rm0, fb1, pb1, mb1, rf1, rp1, rm1,
    a_send, a_recv, o_send, o_recv, s_send, s_recv, g_send, g_recv, h_send, h_recv, k_send, k_recv, e_send, c_send, c_recv, p_send, p_recv,
    x_sem, gain, qb, kb, pos, seg, freq, gain_row, i_sem,
):
    b, t, x, zl, c, y, zh = coords()
    wide_bufs, narrow_bufs = (fb0, pb0, mb0, rf0, rp0, rm0), (fb1, pb1, mb1, rf1, rp1, rm1)
    hl = t % 2
    main = Gather(lambda k, p: w.at[k, pl.ds(pl.multiple_of((zh + p) % 4 * 80, 80), 80)], 4, g_send, g_recv)
    outw = Gather(lambda k, p: wog.at[k, :, pl.ds(p * 512, 512)], 2, h_send, h_recv)

    def kv_at(k, p):
        lane = pl.multiple_of(128 * ((hl + p // 2) % 2), 128)
        return kvg.at[k, pl.ds(256 * (p % 2), 256), pl.ds(lane, 128)]

    keys = Gather(kv_at, 4, k_send, k_recv)
    tgt_blk = blk_of(x, y // 2, y % 2)
    tgt_tp = [yb * 4 + 2 * zl + c for yb in range(4)]
    src_blk = blk_of(x, zh // 2, zh % 2)
    src_tp = [(2 * zl + c) * 4 + k for k in range(4)]

    def other(kb, kt):
        return jnp.logical_or(kb != b, kt != t)

    x_copy = pltpu.make_async_copy(x_hbm, xv, x_sem)
    x_copy.start()
    in_copy = [
        pltpu.make_async_copy(src, dst, i_sem.at[k])
        for k, (src, dst) in enumerate(((gain_h, gain), (qb_h, qb), (kb_h, kb), (pos_h, pos), (seg_h, seg), (freq_h, freq)))
    ]
    for copy in in_copy:
        copy.start()
    for k in range(1, 16):
        signal({"blk": b, "tp": (t + k) % 16})
        signal({"blk": (b + k) % 16, "tp": t})
    for k in range(4):
        @pl.when(other(tgt_blk, tgt_tp[k]))
        def _():
            signal({"blk": tgt_blk, "tp": tgt_tp[k]})

        @pl.when(other(src_blk, src_tp[k]))
        def _():
            signal({"blk": src_blk, "tp": src_tp[k]})
    loop = jnp.logical_and(y == 2 * zl + c, zh == 2 * zl + c).astype(jnp.int32)
    pl.semaphore_wait(pltpu.get_barrier_semaphore(), 38 - 2 * loop)

    def q_src(to):
        return wq.at[:, pl.ds(pl.multiple_of(to * 256, 256), 256)]

    def kv_src(to):
        return wkv.at[:, pl.ds(pl.multiple_of(to * 128, 128), 128)]

    def q_land(k):
        return land.at[k, :, pl.ds(0, 256)]

    def kv_land(k):
        return land.at[k, :, pl.ds(256, 128)]

    for k in range(1, 16):
        to = (y + k) % 4 * 4 + (zh + (0, 3, 1, 2)[k // 4]) % 4
        push(q_src(to), q_land(t), a_send.at[0, k], a_recv.at[0, t], {"blk": b, "tp": to})
        push(kv_src(to), kv_land(t), a_send.at[1, k], a_recv.at[1, t], {"blk": b, "tp": to})
    pltpu.make_async_copy(q_src(t), q_land(t), a_recv.at[0, t]).start()
    pltpu.make_async_copy(kv_src(t), kv_land(t), a_recv.at[1, t]).start()

    def send_segs():
        in_copy[4].wait()
        for k in range(1, 16):
            push(seg, segs.at[b], s_send.at[k], s_recv.at[b], {"blk": (b + k) % 16, "tp": t})
        segs[b] = seg[...]


    in_copy[0].wait()
    for k in range(D // 256):
        gain_row[:, k * 256 : (k + 1) * 256] = gain[k * 256 : (k + 1) * 256].astype(F32)[None, :]
    x_copy.wait()

    def squares(i, carry):
        rows = pl.ds(pl.multiple_of(i * 64, 64), 64)
        total = jnp.zeros((64, 128), F32)
        for j in range(D // 128):
            v = xv[rows, j * 128 : (j + 1) * 128].astype(F32)
            total = total + v * v
        square = jnp.maximum(jnp.sum(total, axis=1, keepdims=True) * (1.0 / D), NORM_FLOOR)
        trig[0, rows, :] = jnp.broadcast_to(lax.rsqrt(square), (64, 128))
        return carry

    lax.fori_loop(0, TOK // 64, squares, 0)

    def turn(i, carry):
        for k in range(5):
            at = pl.ds(pl.multiple_of(i * 640 + k * 128, 128), 128)
            v = xv[:, at].astype(F32) * trig[0] * gain_row[:, at]
            five[k * 128 : (k + 1) * 128, :] = v.astype(BF).astype(F32).T
        for k in range(32):
            slot[i * 32 + k] = five[k * ROWS : (k + 1) * ROWS, :]
        return carry

    lax.fori_loop(0, 8, turn, 0)

    def back(i):
        for k in range(32):
            f = k // 16 * 16 + k % 4 * 4 + k // 4 % 4
            five[k * ROWS : (k + 1) * ROWS, :] = slot[dm[i * 32 + f]]
        for k in range(5):
            ordered[:, k * 128 : (k + 1) * 128] = five[k * 128 : (k + 1) * 128, :].T.astype(BF)

    def group(g):
        zs = (zh + g) % 4
        for k in range(4):
            frm = 4 * k + zs
            landed(q_land(frm), a_recv.at[0, frm])
            landed(kv_land(frm), a_recv.at[1, frm])
            wide[k * ROWS : (k + 1) * ROWS, :] = land[frm].astype(F32)
        w[b, pl.ds(pl.multiple_of(zs * 80, 80), 80), :] = wide[...].astype(BF)
        main.mine(g)

    def send_out():
        for k in range(4):
            src = wo.at[:, pl.ds(k * 1024, 1024)]

            @pl.when(other(tgt_blk, tgt_tp[k]))
            def _():
                push(src, land_o.at[zh], o_send.at[k], o_recv.at[zh], {"blk": tgt_blk, "tp": tgt_tp[k]})

            @pl.when(jnp.logical_not(other(tgt_blk, tgt_tp[k])))
            def _():
                pltpu.make_async_copy(src, land_o.at[zh], o_recv.at[zh]).start()

    def squeeze_out():
        for k in range(4):
            landed(land_o.at[k], o_recv.at[k])
            wide_o[k * ROWS : (k + 1) * ROWS, :] = land_o[k].astype(F32)
        wog[b] = wide_o[...].astype(BF)
        outw.own_z(0, 1)

    group(0)
    group(1)
    main.zfwd(0)
    group(3)
    group(2)
    send_segs()
    send_out()
    acc_w[...] = jnp.zeros((TOK, WC), F32)

    for k in (1, 2, 3, 5):
        in_copy[k].wait()
    angle = freq[...] * pos[...].astype(F32)
    cos_t, sin_t = cos_sin(angle)
    trig[0] = jnp.concatenate([cos_t, cos_t], axis=0).T
    trig[1] = jnp.concatenate([-sin_t, sin_t], axis=0).T
    window = pl.ds(pl.multiple_of(128 * ((5 * t) // 2), 128), 384)
    res[...] = xv[:, window].astype(F32).T


    def mul(i):
        pair = pick(main.order, i) // 2
        back(pair)
        acc_w[...] += jnp.dot(ordered[...], w[pl.ds(pair * 2, 2)].reshape(640, WC), preferred_element_type=F32)

    run(8, mul, {
        0: seq((main.side, False, 0), (main.zfwd, 1), (main.sibs, 0)),
        1: seq((main.zfwd, 3), (main.zfwd, 2), (main.side, False, 1), (main.sibs, 1)),
        2: seq((main.side, True, 0), (main.side, False, 3), (main.side, False, 2), (main.sibs, 2)),
        3: seq((main.far, False, 0), (main.side, True, 1), (main.sibs, 3)),
        4: seq((main.far, False, 1), (main.side, True, 3), (main.side, True, 2), (main.sibs, 4)),
        5: seq((main.far, False, 3), (main.far, False, 2), (squeeze_out,), (main.sibs, 5)),
        6: seq((main.far, True, 0), (main.far, True, 1), (main.sibs, 6)),
        7: seq((main.far, True, 3), (main.far, True, 2), (main.sibs, 7)),
    })

    line = lax.broadcasted_iota(jnp.int32, (HD, TOK), 0)

    is_key = hl == 0
    kv_pair = kb[pl.ds(pl.multiple_of(t // 2 * 256, 256), 256)].astype(F32)[None, :]
    kv_bias = jnp.where(is_key, kv_pair[:, :HD], kv_pair[:, HD:])
    q_bias = qb[pl.ds(pl.multiple_of(t * 256, 256), 256)].astype(F32)[None, :]
    u = acc_w[:, 256:384] + kv_bias
    turned = u * trig[0] + pltpu.roll(u, HD // 2, 1) * trig[1]
    mine = pl.ds(pl.multiple_of(hl * 128, 128), 128)
    kvg[b, :, mine] = jnp.where(is_key, turned, u).astype(BF)
    partner = {"blk": b, "tp": t + 1 - 2 * hl}
    for r in range(2):
        push(kv_at(b, r), kv_at(b, r), e_send.at[r], k_recv.at[b, 2 + r], partner)
        keys.mine(r)
    own_seg = jnp.broadcast_to(seg[...].astype(F32), (HD, TOK))
    own_seg = jnp.where(line == 0, own_seg, jnp.where(line == 1, 1.0, 0.0)).T.astype(BF)
    for h in range(2):
        u = acc_w[:, h * HD : (h + 1) * HD] + q_bias[:, h * HD : (h + 1) * HD]
        u = (u * trig[0] + pltpu.roll(u, HD // 2, 1) * trig[1]).astype(BF)
        for r in range(2):
            q[r, h * 256 : (h + 1) * 256, 0:HD] = u[r * 256 : (r + 1) * 256]
            q[r, h * 256 : (h + 1) * 256, HD:] = own_seg[r * 256 : (r + 1) * 256]

    coef = HD ** -0.5 * LOG2E
    half = TOK // 2

    def column(j, carry):
        @pl.when(j != b)
        def _():
            landed(segs.at[j], s_recv.at[j])

        row = jnp.where(segs[j] == 0, NEGATIVE_FILL, 0.0)
        later = jnp.where(j // 2 > b // 2, NEGATIVE_FILL, 0.0)
        kaug[j] = jnp.where(
            line == 0, jnp.broadcast_to(row, (HD, TOK)), jnp.where(line == 1, later, 0.0)
        ).T.astype(BF)
        return carry

    lax.fori_loop(0, 16, column, 0)

    def block(pair, r, first):
        ss = []
        for k in range(2):
            j = 2 * pair + k
            kop = jnp.concatenate([kvg[j, :, 0:HD], kaug[j]], axis=1)
            v = lax.dot_general(q[r], kop, (((1,), (1,)), ((), ())), preferred_element_type=F32)
            if first:
                qi = lax.broadcasted_iota(jnp.int32, (TOK, TOK), 0) % half + r * half + c * TOK
                ki = lax.broadcasted_iota(jnp.int32, (TOK, TOK), 1) + k * TOK
                v = jnp.where(ki <= qi, v, NEGATIVE_FILL)
            ss += [v[:, i * HD : (i + 1) * HD] for i in range(4)]
        top = ss
        while len(top) > 1:
            top = [jnp.maximum(top[i], top[i + 1]) for i in range(0, len(top), 2)]
        new = jnp.broadcast_to(jnp.max(top[0], axis=1, keepdims=True), (TOK, HD))
        if not first:
            old = m_s[r]
            new = jnp.maximum(old, new)
            factor = jnp.exp2((old - new) * coef)
        o = jnp.zeros((TOK, 2 * HD), F32)
        for k in range(2):
            e = jnp.concatenate([jnp.exp2((ss[4 * k + i] - new) * coef).astype(BF) for i in range(4)], axis=1)
            vop = jnp.concatenate([kvg[2 * pair + k, :, HD:], jnp.ones((TOK, HD), BF)], axis=1)
            o = o + jnp.dot(e, vop, preferred_element_type=F32)
        m_s[r] = new
        if first:
            acc_s[r] = o
        else:
            acc_s[r, :, 0:HD] = acc_s[r, :, 0:HD] * factor + o[:, 0:HD]
            acc_s[r, :, HD:] = acc_s[r, :, HD:] * factor + o[:, HD:]

    keys.side(False, 0, 1)
    for r in range(2):
        keys.wait(b, 2 + r)
        keys.mine(2 + r)
    keys.zfwd(0, 1)
    keys.sibs(0)
    block(b // 2, 0, True)
    block(b // 2, 1, True)
    keys.zfwd(2, 3)
    keys.side(False, 2, 3)
    keys.side(True, 0, 1)
    keys.sibs(1)

    @pl.when(keys.z < b)
    def _():
        block(keys.z // 2, 0, False)
        block(keys.z // 2, 1, False)

    def double(i):
        one = pick(keys.order[2::2], i % 3) // 2
        two = pick(keys.order[3::2], i % 3) // 2

        @pl.when(jnp.minimum(one, two) < b // 2)
        def _():
            block(one, i // 3, False)
            block(two, i // 3, False)

    up, down, opp = (zh + 1) % 4, (zh + 3) % 4, (zh + 2) % 4
    yp, ym, y2 = (y + 1) % 4, (y + 3) % 4, (y + 2) % 4
    zdev = lambda k: {"blk": b, "tp": y * 4 + k}
    ydev = lambda k: {"blk": b, "tp": k * 4 + zh}
    at = lambda k, p: cg.at[k, pl.ds(p * 64, 64)]
    part = TOK // 4

    def waitc(k, p):
        landed(at(k, p), c_recv.at[k, p])

    def mine_c(r):
        rows = pl.ds(r * half, half)
        for h in range(2):
            hr = pl.ds(h * half, half)
            cg[zh, rows, h * HD : (h + 1) * HD] = (acc_s[r, hr, 0:HD] / acc_s[r, hr, HD:]).astype(BF)
        for p in range(4 * r, 4 * r + 4):
            push(at(zh, p), at(zh, p), c_send.at[0, p], c_recv.at[zh, p], zdev(up))
            push(at(zh, p), at(zh, p), c_send.at[1, p], c_recv.at[zh, p], zdev(down))

    def fwd_c(*quarters):
        for r in quarters:
            waitc(down, 2 * r)
            push(at(down, 2 * r), at(down, 2 * r), c_send.at[2, 2 * r], c_recv.at[down, 2 * r], zdev(up))
            waitc(up, 2 * r + 1)
            push(at(up, 2 * r + 1), at(up, 2 * r + 1), c_send.at[2, 2 * r + 1], c_recv.at[up, 2 * r + 1], zdev(down))

    run(6, double, {
        0: seq((keys.side, True, 2), (keys.far, False, 0, 1), (keys.sibs, 2), (keys.sibs, 3)),
        1: seq((keys.side, True, 3), (keys.far, False, 2, 3), (keys.far, True, 0), (keys.sibs, 4), (keys.sibs, 5)),
        2: seq((keys.far, True, 1, 2, 3), (outw.z_in, 0, 1), (outw.own_x, 0, 1), (outw.z_out, 0, 1), (keys.sibs, 6), (keys.sibs, 7)),
        3: seq((mine_c, 0),),
        4: seq((outw.side, False, 0, 1)),
        5: seq((fwd_c, 0), (outw.side, True, 0, 1)),
    })
    mine_c(1)
    fwd_c(1)
    outw.far(False, 0, 1)
    outw.far(True, 0, 1)
    for k in range(8):
        outw.sibs(k)

    parts = ((0, 256), (256, 128), (384, 128))
    far_b, plus, minus, r_far, r_plus, r_minus = [
        [wide_buf] + [narrow_buf.at[k] for k in range(2)]
        for wide_buf, narrow_buf in zip(wide_bufs, narrow_bufs)
    ]

    def partial(k, r):
        start, n = parts[r]
        v = jnp.zeros((320, n), F32)
        for i in range(4):
            v = v + lax.dot_general(
                wog[pl.ds(k * 4, 4), :, i * 256 : (i + 1) * 256].reshape(320, 256),
                cg[i, pl.ds(start, n), :],
                (((1,), (1,)), ((), ())),
                preferred_element_type=F32,
            )
        return v

    lo, hi = pl.ds(0, 160), pl.ds(160, 160)
    kept = {}

    def scatter_far(r):
        for k in ((0, 1), (2,), (3,))[r]:
            waitc(down, 2 * k + 1)
            waitc(up, 2 * k)
            waitc(opp, 2 * k)
            waitc(opp, 2 * k + 1)
        far_b[r][...] = partial(y2, r).astype(BF)
        push(far_b[r].at[lo], r_far[r].at[lo], p_send.at[r, 0], p_recv.at[r, 0], ydev(yp))
        push(far_b[r].at[hi], r_far[r].at[hi], p_send.at[r, 1], p_recv.at[r, 1], ydev(ym))

    def scatter_mid(r):
        v = partial(yp, r)
        plus[r][hi, :] = v[160:].astype(BF)
        push(plus[r].at[hi], r_plus[r].at[hi], p_send.at[r, 2], p_recv.at[r, 2], ydev(yp))
        u = partial(ym, r)
        minus[r][lo, :] = u[:160].astype(BF)
        push(minus[r].at[lo], r_minus[r].at[lo], p_send.at[r, 3], p_recv.at[r, 3], ydev(ym))
        kept[r] = v[:160], u[160:]

    def scatter_near(r):
        v, u = kept[r]
        landed(r_far[r].at[lo], p_recv.at[r, 0])
        plus[r][lo, :] = (v + r_far[r][lo, :].astype(F32)).astype(BF)
        push(plus[r].at[lo], r_plus[r].at[lo], p_send.at[r, 4], p_recv.at[r, 4], ydev(yp))
        landed(r_far[r].at[hi], p_recv.at[r, 1])
        minus[r][hi, :] = (u + r_far[r][hi, :].astype(F32)).astype(BF)
        push(minus[r].at[hi], r_minus[r].at[hi], p_send.at[r, 5], p_recv.at[r, 5], ydev(ym))

    def keep(r):
        cols = pl.ds(*parts[r])
        res[pl.ds(0, 320), cols] = partial(y, r) + res[pl.ds(pl.multiple_of(64 * hl, 64), 320), cols]

    def finish(r):
        for sl, k1, k2 in ((hi, 2, 5), (lo, 4, 3)):
            landed(r_plus[r].at[sl], p_recv.at[r, k1])
            landed(r_minus[r].at[sl], p_recv.at[r, k2])
        cols = pl.ds(*parts[r])
        out[:, cols] = (res[pl.ds(0, 320), cols] + r_plus[r][...].astype(F32) + r_minus[r][...].astype(F32)).astype(BF)

    scatter_far(0)
    scatter_mid(0)
    keep(0)
    fwd_c(2)
    fwd_c(3)
    scatter_near(0)
    scatter_far(1)
    scatter_far(2)
    scatter_mid(1)
    scatter_mid(2)
    scatter_near(1)
    keep(1)
    scatter_near(2)
    keep(2)
    finish(0)
    finish(1)
    finish(2)

    for k in range(1, 16):
        landed(q_land(0), a_send.at[0, k])
        landed(kv_land(0), a_send.at[1, k])
        landed(segs.at[0], s_send.at[k])
    for k in range(4):
        @pl.when(other(tgt_blk, tgt_tp[k]))
        def _():
            landed(land_o.at[k], o_send.at[k])

    for k in range(8):
        for i in range(3):
            landed(at(0, 0), c_send.at[i, k])
    for r in range(2):
        landed(kv_at(0, r), e_send.at[r])
    for r in range(3):
        for k in range(6):
            landed(far_b[r].at[lo], p_send.at[r, k])
    main.drain()
    outw.drain()
    keys.drain()


def per_device(residual_in, norm_gain, w_query, w_key_value, query_bias, key_value_bias, w_output, device_map, positions, segments):
    freq = (np.float64(ROPE_BASE) ** (-np.arange(HD // 2) * 2.0 / HD)).astype(np.float32)[:, None]
    freq = jnp.asarray(np.repeat(freq, TOK, axis=1))
    hbm = pl.BlockSpec(memory_space=pl.ANY)
    vm = pl.BlockSpec(memory_space=VM)
    turned = pl.pallas_call(
        layer,
        out_shape=jax.ShapeDtypeStruct((320, TOK), BF),
        in_specs=[pl.BlockSpec(memory_space=pltpu.SMEM), hbm, hbm, hbm, hbm, hbm, hbm, hbm, hbm, hbm, hbm],
        out_specs=vm,
        scratch_shapes=[
            VM((TOK, D), BF),
            VM((256, ROWS, TOK), F32),
            VM((640, TOK), F32),
            VM((TOK, 640), BF),
            VM((16, ROWS, WC), BF),
            VM((80, WC), F32),
            VM((16, 320, WC), BF),
            VM((4, ROWS, 1024), BF),
            VM((80, 1024), F32),
            VM((16, 80, 1024), BF),
            VM((16, 1, TOK), jnp.int32),
            VM((16, TOK, HD), BF),
            VM((TOK, WC), F32),
            VM((2, TOK, HD), F32),
            VM((384, TOK), F32),
            VM((2, TOK, 256), BF),
            VM((16, TOK, 256), BF),
            VM((2, TOK, HD), F32),
            VM((2, TOK, 256), F32),
            VM((4, TOK, 256), BF),
        ]
        + [VM((320, 256), BF)] * 6
        + [VM((2, 320, 128), BF)] * 6
        + [
            DMA((2, 16)), DMA((2, 16)), DMA((4,)), DMA((4,)), DMA((16,)), DMA((16,)),
            DMA((sends_of(4),)), DMA((16, 4)), DMA((sends_of(2),)), DMA((16, 2)), DMA((sends_of(4),)), DMA((16, 4)), DMA((2,)),
            DMA((3, 8)), DMA((4, 8)), DMA((3, 6)), DMA((3, 6)), DMA,
            VM((D,), BF), VM((4096,), BF), VM((2048,), BF), VM((1, TOK), jnp.int32), VM((1, TOK), jnp.int32), VM((HD // 2, TOK), F32), VM((1, D), F32),
            DMA((6,)),
        ],
        compiler_params=pltpu.CompilerParams(collective_id=0, has_side_effects=True, vmem_limit_bytes=VLIM),
        name="layer",
    )(
        device_map, residual_in, w_query, w_key_value, w_output.T, norm_gain, query_bias, key_value_bias,
        positions[None, :], segments[None, :], freq,
    )
    return turned.T


def solution(mesh):
    both = ("blk", "tp")
    placed = (P("blk", None), P(), P(both, None), P(both, None), P(), P(), P(None, both), P(), P("blk"), P("blk"))
    return jax.shard_map(per_device, mesh=mesh, in_specs=placed, out_specs=P("blk", "tp"), check_vma=False)
```

```python
import jax
import jax.numpy as jnp
import numpy as np
from jax import lax
from jax.experimental import pallas as pl
from jax.experimental.pallas import tpu as pltpu
from jax.sharding import PartitionSpec as P

D = 5120
HD = 128
TOK = 512
ROWS = 20
WC = 384
NORM_FLOOR = 0.0625
ROPE_BASE = 1000000.0
NEGATIVE_FILL = -1e30
LOG2E = 1.4426950408889634
MESH = pl.DeviceIdType.MESH
VM = pltpu.VMEM
DMA = pltpu.SemaphoreType.DMA
BF = jnp.bfloat16
F32 = jnp.float32
VLIM = 62 * 1024 * 1024
PIO2 = (1.5703125, 4.83751296997e-04, 7.54978995489e-08)


def coords():
    b = lax.axis_index("blk")
    t = lax.axis_index("tp")
    return b, t, b // 4, (b // 2) % 2, b % 2, t // 4, t % 4


def blk_of(x, zl, c):
    return x * 4 + zl * 2 + c


def signal(dev):
    pl.semaphore_signal(pltpu.get_barrier_semaphore(), inc=1, device_id=dev, device_id_type=MESH)


def push(src, dst, ssem, rsem, dev):
    pltpu.make_async_remote_copy(src, dst, ssem, rsem, device_id=dev, device_id_type=MESH).start()


def landed(ref, sem):
    pltpu.make_async_copy(ref, ref, sem).wait()


def sends_of(pieces):
    return 15 * pieces


class Gather:
    def __init__(self, at, pieces, send, recv, xfirst=()):
        self.at, self.n, self.send, self.recv, self.xfirst = at, pieces, send, recv, xfirst
        b, t, x, zl, c, y, zh = coords()
        self.t = t
        self.own = b
        self.sib = blk_of(x, zl, 1 - c)
        self.z = blk_of(x, 1 - zl, c)
        xp, xm, x2 = (x + 1) % 4, (x + 3) % 4, (x + 2) % 4
        self.xp, self.xm = blk_of(xp, zl, c), blk_of(xm, zl, c)
        self.xpz, self.xmz = blk_of(xp, 1 - zl, c), blk_of(xm, 1 - zl, c)
        self.x2, self.x2z = blk_of(x2, zl, c), blk_of(x2, 1 - zl, c)
        self.order = (self.own, self.z, self.xm, self.xp, self.xmz, self.xpz, self.x2, self.x2z)
        self.count = 0
        self.sent = []

    def _send(self, chunk, p, to):
        ref = self.at(chunk, p)
        k = self.count
        self.count += 1
        push(ref, ref, self.send.at[k], self.recv.at[chunk, p], {"blk": to, "tp": self.t})
        self.sent.append((p, k))

    def wait(self, chunk, p):
        landed(self.at(chunk, p), self.recv.at[chunk, p])

    def own_z(self, *pieces):
        for p in pieces:
            for to in (self.z, self.sib):
                self._send(self.own, p, to)

    def own_x(self, *pieces):
        for p in pieces:
            for to in (self.xp, self.xm):
                self._send(self.own, p, to)

    def mine(self, *pieces):
        for p in pieces:
            self.own_x(p)
            self.own_z(p)

    def z_in(self, *pieces):
        for p in pieces:
            self.wait(self.z, p)
            self._send(self.z, p, self.sib)

    def z_out(self, *pieces):
        for p in pieces:
            for to in (self.xp, self.xm):
                self._send(self.z, p, to)

    def zfwd(self, *pieces):
        for p in pieces:
            self.wait(self.z, p)
            if p not in self.xfirst:
                self.z_out(p)
            self._send(self.z, p, self.sib)

    def side(self, zside, *pieces):
        minus, plus = (self.xmz, self.xpz) if zside else (self.xm, self.xp)
        for p in pieces:
            for chunk, on, even in ((minus, self.xp, 0), (plus, self.xm, 1)):
                self.wait(chunk, p)
                if p % 2 == even and not (zside and p in self.xfirst):
                    self._send(chunk, p, on)
                if p in self.xfirst and not zside:
                    self._send(chunk, p, self.z)
                self._send(chunk, p, self.sib)

    def far(self, zside, *pieces):
        chunk = self.x2z if zside else self.x2
        for p in pieces:
            self.wait(chunk, p)
            if p in self.xfirst and not zside:
                self._send(chunk, p, self.z)
            self._send(chunk, p, self.sib)

    def sibs(self, k):
        chunk = flip(self.order[k])
        for p in range(self.n):
            self.wait(chunk, p)

    def drain(self):
        for p, k in self.sent:
            landed(self.at(0, p), self.send.at[k])


def flip(k):
    return k + 1 - 2 * (k % 2)


def pick(options, i):
    r = options[0]
    for k in range(1, len(options)):
        r = jnp.where(i == k, options[k], r)
    return r


def run(n, compute, events):
    def body(i, carry):
        for k, event in events.items():
            pl.when(i == k)(event)
        compute(i)
        return carry

    lax.fori_loop(0, n, body, 0)


def seq(*calls):
    def go():
        for f, *args in calls:
            f(*args)

    return go


def cos_sin(angle):
    k = jnp.floor(angle * (2.0 / np.pi) + 0.5)
    r = ((angle - k * PIO2[0]) - k * PIO2[1]) - k * PIO2[2]
    s = r * r
    sin = r + r * s * (-1.6666654611e-1 + s * (8.3321608736e-3 + s * -1.9515295891e-4))
    cos = 1.0 - 0.5 * s + s * s * (4.166664568298827e-2 + s * (-1.388731625493765e-3 + s * 2.443315711809948e-5))
    m = k.astype(jnp.int32)
    odd = m % 2 == 1
    cos_v = jnp.where(odd, sin, cos)
    sin_v = jnp.where(odd, cos, sin)
    cos_v = jnp.where((m + 1) // 2 % 2 == 1, -cos_v, cos_v)
    sin_v = jnp.where(m // 2 % 2 == 1, -sin_v, sin_v)
    return cos_v, sin_v


def layer(
    dm, x_hbm, wq, wkv, wo, gain_h, qb_h, kb_h, pos_h, seg_h, freq_h,
    out,
    xv, slot, five, ordered, land, wide, w, land_o, wide_o, wog, segs, kaug, acc_w, trig, res, q, kvg, m_s, acc_s, cg,
    fb0, pb0, mb0, rf0, rp0, rm0, fb1, pb1, mb1, rf1, rp1, rm1,
    a_send, a_recv, o_send, o_recv, s_send, s_recv, g_send, g_recv, h_send, h_recv, k_send, k_recv, e_send, c_send, c_recv, p_send, p_recv,
    x_sem, gain, qb, kb, pos, seg, freq, gain_row, i_sem,
):
    b, t, x, zl, c, y, zh = coords()
    wide_bufs, narrow_bufs = (fb0, pb0, mb0, rf0, rp0, rm0), (fb1, pb1, mb1, rf1, rp1, rm1)
    hl = t % 2
    main = Gather(lambda k, p: w.at[k, pl.ds(pl.multiple_of((zh + p) % 4 * 80, 80), 80)], 4, g_send, g_recv)
    outw = Gather(lambda k, p: wog.at[k, :, pl.ds(p * 512, 512)], 2, h_send, h_recv)

    def kv_at(k, p):
        lane = pl.multiple_of(128 * ((hl + p // 2) % 2), 128)
        return kvg.at[k, pl.ds(256 * (p % 2), 256), pl.ds(lane, 128)]

    keys = Gather(kv_at, 4, k_send, k_recv)
    tgt_blk = blk_of(x, y // 2, y % 2)
    tgt_tp = [yb * 4 + 2 * zl + c for yb in range(4)]
    src_blk = blk_of(x, zh // 2, zh % 2)
    src_tp = [(2 * zl + c) * 4 + k for k in range(4)]

    def other(kb, kt):
        return jnp.logical_or(kb != b, kt != t)

    x_copy = pltpu.make_async_copy(x_hbm, xv, x_sem)
    x_copy.start()
    in_copy = [
        pltpu.make_async_copy(src, dst, i_sem.at[k])
        for k, (src, dst) in enumerate(((gain_h, gain), (qb_h, qb), (kb_h, kb), (pos_h, pos), (seg_h, seg), (freq_h, freq)))
    ]
    for copy in in_copy:
        copy.start()
    for k in range(1, 16):
        signal({"blk": b, "tp": (t + k) % 16})
        signal({"blk": (b + k) % 16, "tp": t})
    for k in range(4):
        @pl.when(other(tgt_blk, tgt_tp[k]))
        def _():
            signal({"blk": tgt_blk, "tp": tgt_tp[k]})

        @pl.when(other(src_blk, src_tp[k]))
        def _():
            signal({"blk": src_blk, "tp": src_tp[k]})
    loop = jnp.logical_and(y == 2 * zl + c, zh == 2 * zl + c).astype(jnp.int32)
    pl.semaphore_wait(pltpu.get_barrier_semaphore(), 38 - 2 * loop)

    def q_src(to):
        return wq.at[:, pl.ds(pl.multiple_of(to * 256, 256), 256)]

    def kv_src(to):
        return wkv.at[:, pl.ds(pl.multiple_of(to * 128, 128), 128)]

    def q_land(k):
        return land.at[k, :, pl.ds(0, 256)]

    def kv_land(k):
        return land.at[k, :, pl.ds(256, 128)]

    for k in range(1, 16):
        to = (y + k) % 4 * 4 + (zh + (0, 3, 1, 2)[k // 4]) % 4
        push(q_src(to), q_land(t), a_send.at[0, k], a_recv.at[0, t], {"blk": b, "tp": to})
        push(kv_src(to), kv_land(t), a_send.at[1, k], a_recv.at[1, t], {"blk": b, "tp": to})
    pltpu.make_async_copy(q_src(t), q_land(t), a_recv.at[0, t]).start()
    pltpu.make_async_copy(kv_src(t), kv_land(t), a_recv.at[1, t]).start()

    def send_segs():
        in_copy[4].wait()
        for k in range(1, 16):
            push(seg, segs.at[b], s_send.at[k], s_recv.at[b], {"blk": (b + k) % 16, "tp": t})
        segs[b] = seg[...]


    in_copy[0].wait()
    for k in range(D // 256):
        gain_row[:, k * 256 : (k + 1) * 256] = gain[k * 256 : (k + 1) * 256].astype(F32)[None, :]
    x_copy.wait()

    def squares(i, carry):
        rows = pl.ds(pl.multiple_of(i * 64, 64), 64)
        total = jnp.zeros((64, 128), F32)
        for j in range(D // 128):
            v = xv[rows, j * 128 : (j + 1) * 128].astype(F32)
            total = total + v * v
        square = jnp.maximum(jnp.sum(total, axis=1, keepdims=True) * (1.0 / D), NORM_FLOOR)
        trig[0, rows, :] = jnp.broadcast_to(lax.rsqrt(square), (64, 128))
        return carry

    lax.fori_loop(0, TOK // 64, squares, 0)

    def turn(i, carry):
        for k in range(5):
            at = pl.ds(pl.multiple_of(i * 640 + k * 128, 128), 128)
            v = xv[:, at].astype(F32) * trig[0] * gain_row[:, at]
            five[k * 128 : (k + 1) * 128, :] = v.astype(BF).astype(F32).T
        for k in range(32):
            slot[i * 32 + k] = five[k * ROWS : (k + 1) * ROWS, :]
        return carry

    lax.fori_loop(0, 8, turn, 0)

    def back(i):
        for k in range(32):
            f = k // 16 * 16 + k % 4 * 4 + k // 4 % 4
            five[k * ROWS : (k + 1) * ROWS, :] = slot[dm[i * 32 + f]]
        for k in range(5):
            ordered[:, k * 128 : (k + 1) * 128] = five[k * 128 : (k + 1) * 128, :].T.astype(BF)

    def group(g):
        zs = (zh + g) % 4
        for k in range(4):
            frm = 4 * k + zs
            landed(q_land(frm), a_recv.at[0, frm])
            landed(kv_land(frm), a_recv.at[1, frm])
            wide[k * ROWS : (k + 1) * ROWS, :] = land[frm].astype(F32)
        w[b, pl.ds(pl.multiple_of(zs * 80, 80), 80), :] = wide[...].astype(BF)
        main.mine(g)

    def send_out():
        for k in range(4):
            src = wo.at[:, pl.ds(k * 1024, 1024)]

            @pl.when(other(tgt_blk, tgt_tp[k]))
            def _():
                push(src, land_o.at[zh], o_send.at[k], o_recv.at[zh], {"blk": tgt_blk, "tp": tgt_tp[k]})

            @pl.when(jnp.logical_not(other(tgt_blk, tgt_tp[k])))
            def _():
                pltpu.make_async_copy(src, land_o.at[zh], o_recv.at[zh]).start()

    def squeeze_out():
        for k in range(4):
            landed(land_o.at[k], o_recv.at[k])
            wide_o[k * ROWS : (k + 1) * ROWS, :] = land_o[k].astype(F32)
        wog[b] = wide_o[...].astype(BF)
        outw.own_z(0, 1)

    group(0)
    group(1)
    main.zfwd(0)
    group(3)
    group(2)
    acc_w[...] = jnp.zeros((TOK, WC), F32)

    def rope_tables():
        for k in (1, 2, 3, 5):
            in_copy[k].wait()
        cos_t, sin_t = cos_sin(freq[...] * pos[...].astype(F32))
        trig[0] = jnp.concatenate([cos_t, cos_t], axis=0).T
        trig[1] = jnp.concatenate([-sin_t, sin_t], axis=0).T

    def mul(i):
        pair = pick(main.order, i) // 2
        back(pair)
        acc_w[...] += jnp.dot(ordered[...], w[pl.ds(pair * 2, 2)].reshape(640, WC), preferred_element_type=F32)

    run(8, mul, {
        0: seq((main.side, False, 0), (main.zfwd, 1), (main.sibs, 0)),
        1: seq((rope_tables,), (main.side, False, 1), (main.zfwd, 3), (main.zfwd, 2), (main.sibs, 1)),
        2: seq((send_segs,), (send_out,), (main.side, True, 0), (main.side, False, 3), (main.side, False, 2), (main.sibs, 2)),
        3: seq((main.far, False, 0), (main.side, True, 1), (main.sibs, 3)),
        4: seq((main.far, False, 1), (main.side, True, 3), (main.side, True, 2), (main.sibs, 4)),
        5: seq((main.far, False, 3), (main.far, False, 2), (main.sibs, 5)),
        6: seq((main.far, True, 0), (main.far, True, 1), (main.sibs, 6)),
        7: seq((main.far, True, 3), (main.far, True, 2), (main.sibs, 7)),
    })

    line = lax.broadcasted_iota(jnp.int32, (HD, TOK), 0)

    is_key = hl == 0
    kv_pair = kb[pl.ds(pl.multiple_of(t // 2 * 256, 256), 256)].astype(F32)[None, :]
    kv_bias = jnp.where(is_key, kv_pair[:, :HD], kv_pair[:, HD:])
    q_bias = qb[pl.ds(pl.multiple_of(t * 256, 256), 256)].astype(F32)[None, :]
    u = acc_w[:, 256:384] + kv_bias
    turned = u * trig[0] + pltpu.roll(u, HD // 2, 1) * trig[1]
    mine = pl.ds(pl.multiple_of(hl * 128, 128), 128)
    kvg[b, :, mine] = jnp.where(is_key, turned, u).astype(BF)
    partner = {"blk": b, "tp": t + 1 - 2 * hl}
    for r in range(2):
        push(kv_at(b, r), kv_at(b, r), e_send.at[r], k_recv.at[b, 2 + r], partner)
        keys.mine(r)
    own_seg = jnp.broadcast_to(seg[...].astype(F32), (HD, TOK))
    own_seg = jnp.where(line == 0, own_seg, jnp.where(line == 1, 1.0, 0.0)).T.astype(BF)
    for h in range(2):
        u = acc_w[:, h * HD : (h + 1) * HD] + q_bias[:, h * HD : (h + 1) * HD]
        u = (u * trig[0] + pltpu.roll(u, HD // 2, 1) * trig[1]).astype(BF)
        for r in range(2):
            q[r, h * 256 : (h + 1) * 256, 0:HD] = u[r * 256 : (r + 1) * 256]
            q[r, h * 256 : (h + 1) * 256, HD:] = own_seg[r * 256 : (r + 1) * 256]

    coef = HD ** -0.5 * LOG2E
    half = TOK // 2

    def column(j, carry):
        @pl.when(j != b)
        def _():
            landed(segs.at[j], s_recv.at[j])

        row = jnp.where(segs[j] == 0, NEGATIVE_FILL, 0.0)
        later = jnp.where(j // 2 > b // 2, NEGATIVE_FILL, 0.0)
        kaug[j] = jnp.where(
            line == 0, jnp.broadcast_to(row, (HD, TOK)), jnp.where(line == 1, later, 0.0)
        ).T.astype(BF)
        return carry

    lax.fori_loop(0, 16, column, 0)
    squeeze_out()
    window = pl.ds(pl.multiple_of(128 * ((5 * t) // 2), 128), 384)
    res[...] = xv[:, window].astype(F32).T

    def block(pair, r, first):
        ss = []
        for k in range(2):
            j = 2 * pair + k
            kop = jnp.concatenate([kvg[j, :, 0:HD], kaug[j]], axis=1)
            v = lax.dot_general(q[r], kop, (((1,), (1,)), ((), ())), preferred_element_type=F32)
            if first:
                qi = lax.broadcasted_iota(jnp.int32, (TOK, TOK), 0) % half + r * half + c * TOK
                ki = lax.broadcasted_iota(jnp.int32, (TOK, TOK), 1) + k * TOK
                v = jnp.where(ki <= qi, v, NEGATIVE_FILL)
            ss += [v[:, i * HD : (i + 1) * HD] for i in range(4)]
        top = ss
        while len(top) > 1:
            top = [jnp.maximum(top[i], top[i + 1]) for i in range(0, len(top), 2)]
        new = jnp.broadcast_to(jnp.max(top[0], axis=1, keepdims=True), (TOK, HD))
        if not first:
            old = m_s[r]
            new = jnp.maximum(old, new)
            factor = jnp.exp2((old - new) * coef)
        o = jnp.zeros((TOK, 2 * HD), F32)
        for k in range(2):
            e = jnp.concatenate([jnp.exp2((ss[4 * k + i] - new) * coef).astype(BF) for i in range(4)], axis=1)
            vop = jnp.concatenate([kvg[2 * pair + k, :, HD:], jnp.ones((TOK, HD), BF)], axis=1)
            o = o + jnp.dot(e, vop, preferred_element_type=F32)
        m_s[r] = new
        if first:
            acc_s[r] = o
        else:
            acc_s[r, :, 0:HD] = acc_s[r, :, 0:HD] * factor + o[:, 0:HD]
            acc_s[r, :, HD:] = acc_s[r, :, HD:] * factor + o[:, HD:]

    keys.side(False, 0, 1)
    for r in range(2):
        keys.wait(b, 2 + r)
        keys.mine(2 + r)
    keys.zfwd(0, 1)
    keys.sibs(0)
    block(b // 2, 0, True)
    block(b // 2, 1, True)
    keys.zfwd(2, 3)
    keys.side(False, 2, 3)
    keys.side(True, 0, 1)
    keys.sibs(1)

    @pl.when(keys.z < b)
    def _():
        block(keys.z // 2, 0, False)
        block(keys.z // 2, 1, False)

    def double(i):
        one = pick(keys.order[2::2], i % 3) // 2
        two = pick(keys.order[3::2], i % 3) // 2

        @pl.when(jnp.minimum(one, two) < b // 2)
        def _():
            block(one, i // 3, False)
            block(two, i // 3, False)

    up, down, opp = (zh + 1) % 4, (zh + 3) % 4, (zh + 2) % 4
    yp, ym, y2 = (y + 1) % 4, (y + 3) % 4, (y + 2) % 4
    zdev = lambda k: {"blk": b, "tp": y * 4 + k}
    ydev = lambda k: {"blk": b, "tp": k * 4 + zh}
    at = lambda k, p: cg.at[k, pl.ds(p * 64, 64)]
    part = TOK // 4

    def waitc(k, p):
        landed(at(k, p), c_recv.at[k, p])

    def mine_c(r):
        rows = pl.ds(r * half, half)
        for h in range(2):
            hr = pl.ds(h * half, half)
            cg[zh, rows, h * HD : (h + 1) * HD] = (acc_s[r, hr, 0:HD] / acc_s[r, hr, HD:]).astype(BF)
        for p in range(4 * r, 4 * r + 4):
            push(at(zh, p), at(zh, p), c_send.at[0, p], c_recv.at[zh, p], zdev(up))
            push(at(zh, p), at(zh, p), c_send.at[1, p], c_recv.at[zh, p], zdev(down))

    def fwd_c(*quarters):
        for r in quarters:
            waitc(down, 2 * r)
            push(at(down, 2 * r), at(down, 2 * r), c_send.at[2, 2 * r], c_recv.at[down, 2 * r], zdev(up))
            waitc(up, 2 * r + 1)
            push(at(up, 2 * r + 1), at(up, 2 * r + 1), c_send.at[2, 2 * r + 1], c_recv.at[up, 2 * r + 1], zdev(down))

    run(6, double, {
        0: seq((keys.side, True, 2), (keys.far, False, 0, 1), (keys.sibs, 2), (keys.sibs, 3)),
        1: seq((keys.side, True, 3), (outw.own_x, 0, 1), (keys.far, False, 2, 3), (keys.far, True, 0), (keys.sibs, 4), (keys.sibs, 5)),
        2: seq((outw.z_in, 0, 1), (outw.z_out, 0, 1), (keys.far, True, 1, 2, 3), (keys.sibs, 6), (keys.sibs, 7)),
        3: seq((mine_c, 0),),
        4: seq((outw.side, False, 0, 1)),
        5: seq((outw.side, True, 0, 1), (fwd_c, 0, 1)),
    })
    mine_c(1)
    outw.far(False, 0, 1)
    outw.far(True, 0, 1)
    for k in range(8):
        outw.sibs(k)

    parts = ((0, 256), (256, 128), (384, 128))
    far_b, plus, minus, r_far, r_plus, r_minus = [
        [wide_buf] + [narrow_buf.at[k] for k in range(2)]
        for wide_buf, narrow_buf in zip(wide_bufs, narrow_bufs)
    ]

    def partial(k, r):
        start, n = parts[r]
        v = jnp.zeros((320, n), F32)
        for i in range(4):
            v = v + lax.dot_general(
                wog[pl.ds(k * 4, 4), :, i * 256 : (i + 1) * 256].reshape(320, 256),
                cg[i, pl.ds(start, n), :],
                (((1,), (1,)), ((), ())),
                preferred_element_type=F32,
            )
        return v

    lo, hi = pl.ds(0, 160), pl.ds(160, 160)
    kept = {}

    def scatter_far(r):
        for k in ((0, 1), (2,), (3,))[r]:
            waitc(down, 2 * k + 1)
            waitc(up, 2 * k)
            waitc(opp, 2 * k)
            waitc(opp, 2 * k + 1)
        far_b[r][...] = partial(y2, r).astype(BF)
        push(far_b[r].at[lo], r_far[r].at[lo], p_send.at[r, 0], p_recv.at[r, 0], ydev(yp))
        push(far_b[r].at[hi], r_far[r].at[hi], p_send.at[r, 1], p_recv.at[r, 1], ydev(ym))

    def scatter_mid(r):
        v = partial(yp, r)
        plus[r][hi, :] = v[160:].astype(BF)
        push(plus[r].at[hi], r_plus[r].at[hi], p_send.at[r, 2], p_recv.at[r, 2], ydev(yp))
        u = partial(ym, r)
        minus[r][lo, :] = u[:160].astype(BF)
        push(minus[r].at[lo], r_minus[r].at[lo], p_send.at[r, 3], p_recv.at[r, 3], ydev(ym))
        kept[r] = v[:160], u[160:]

    def scatter_near(r):
        v, u = kept[r]
        landed(r_far[r].at[lo], p_recv.at[r, 0])
        plus[r][lo, :] = (v + r_far[r][lo, :].astype(F32)).astype(BF)
        push(plus[r].at[lo], r_plus[r].at[lo], p_send.at[r, 4], p_recv.at[r, 4], ydev(yp))
        landed(r_far[r].at[hi], p_recv.at[r, 1])
        minus[r][hi, :] = (u + r_far[r][hi, :].astype(F32)).astype(BF)
        push(minus[r].at[hi], r_minus[r].at[hi], p_send.at[r, 5], p_recv.at[r, 5], ydev(ym))

    def keep(r):
        cols = pl.ds(*parts[r])
        res[pl.ds(0, 320), cols] = partial(y, r) + res[pl.ds(pl.multiple_of(64 * hl, 64), 320), cols]

    def finish(r):
        for sl, k1, k2 in ((hi, 2, 5), (lo, 4, 3)):
            landed(r_plus[r].at[sl], p_recv.at[r, k1])
            landed(r_minus[r].at[sl], p_recv.at[r, k2])
        cols = pl.ds(*parts[r])
        out[:, cols] = (res[pl.ds(0, 320), cols] + r_plus[r][...].astype(F32) + r_minus[r][...].astype(F32)).astype(BF)

    scatter_far(0)
    scatter_mid(0)
    keep(0)
    fwd_c(2)
    fwd_c(3)
    scatter_near(0)
    scatter_far(1)
    scatter_far(2)
    scatter_mid(1)
    scatter_mid(2)
    scatter_near(1)
    keep(1)
    scatter_near(2)
    keep(2)
    finish(0)
    finish(1)
    finish(2)

    for k in range(1, 16):
        landed(q_land(0), a_send.at[0, k])
        landed(kv_land(0), a_send.at[1, k])
        landed(segs.at[0], s_send.at[k])
    for k in range(4):
        @pl.when(other(tgt_blk, tgt_tp[k]))
        def _():
            landed(land_o.at[k], o_send.at[k])

    for k in range(8):
        for i in range(3):
            landed(at(0, 0), c_send.at[i, k])
    for r in range(2):
        landed(kv_at(0, r), e_send.at[r])
    for r in range(3):
        for k in range(6):
            landed(far_b[r].at[lo], p_send.at[r, k])
    main.drain()
    outw.drain()
    keys.drain()


def per_device(residual_in, norm_gain, w_query, w_key_value, query_bias, key_value_bias, w_output, device_map, positions, segments):
    freq = (np.float64(ROPE_BASE) ** (-np.arange(HD // 2) * 2.0 / HD)).astype(np.float32)[:, None]
    freq = jnp.asarray(np.repeat(freq, TOK, axis=1))
    hbm = pl.BlockSpec(memory_space=pl.ANY)
    vm = pl.BlockSpec(memory_space=VM)
    turned = pl.pallas_call(
        layer,
        out_shape=jax.ShapeDtypeStruct((320, TOK), BF),
        in_specs=[pl.BlockSpec(memory_space=pltpu.SMEM), hbm, hbm, hbm, hbm, hbm, hbm, hbm, hbm, hbm, hbm],
        out_specs=vm,
        scratch_shapes=[
            VM((TOK, D), BF),
            VM((256, ROWS, TOK), F32),
            VM((640, TOK), F32),
            VM((TOK, 640), BF),
            VM((16, ROWS, WC), BF),
            VM((80, WC), F32),
            VM((16, 320, WC), BF),
            VM((4, ROWS, 1024), BF),
            VM((80, 1024), F32),
            VM((16, 80, 1024), BF),
            VM((16, 1, TOK), jnp.int32),
            VM((16, TOK, HD), BF),
            VM((TOK, WC), F32),
            VM((2, TOK, HD), F32),
            VM((384, TOK), F32),
            VM((2, TOK, 256), BF),
            VM((16, TOK, 256), BF),
            VM((2, TOK, HD), F32),
            VM((2, TOK, 256), F32),
            VM((4, TOK, 256), BF),
        ]
        + [VM((320, 256), BF)] * 6
        + [VM((2, 320, 128), BF)] * 6
        + [
            DMA((2, 16)), DMA((2, 16)), DMA((4,)), DMA((4,)), DMA((16,)), DMA((16,)),
            DMA((sends_of(4),)), DMA((16, 4)), DMA((sends_of(2),)), DMA((16, 2)), DMA((sends_of(4),)), DMA((16, 4)), DMA((2,)),
            DMA((3, 8)), DMA((4, 8)), DMA((3, 6)), DMA((3, 6)), DMA,
            VM((D,), BF), VM((4096,), BF), VM((2048,), BF), VM((1, TOK), jnp.int32), VM((1, TOK), jnp.int32), VM((HD // 2, TOK), F32), VM((1, D), F32),
            DMA((6,)),
        ],
        compiler_params=pltpu.CompilerParams(collective_id=0, has_side_effects=True, vmem_limit_bytes=VLIM),
        name="layer",
    )(
        device_map, residual_in, w_query, w_key_value, w_output.T, norm_gain, query_bias, key_value_bias,
        positions[None, :], segments[None, :], freq,
    )
    return turned.T


def solution(mesh):
    both = ("blk", "tp")
    placed = (P("blk", None), P(), P(both, None), P(both, None), P(), P(), P(None, both), P(), P("blk"), P("blk"))
    return jax.shard_map(per_device, mesh=mesh, in_specs=placed, out_specs=P("blk", "tp"), check_vma=False)
```

```python
import jax
import jax.numpy as jnp
import numpy as np
from jax import lax
from jax.experimental import pallas as pl
from jax.experimental.pallas import tpu as pltpu
from jax.sharding import PartitionSpec as P

D = 5120
HD = 128
TOK = 512
ROWS = 20
WC = 384
NORM_FLOOR = 0.0625
ROPE_BASE = 1000000.0
NEGATIVE_FILL = -1e30
LOG2E = 1.4426950408889634
MESH = pl.DeviceIdType.MESH
VM = pltpu.VMEM
DMA = pltpu.SemaphoreType.DMA
BF = jnp.bfloat16
F32 = jnp.float32
VLIM = 62 * 1024 * 1024
PIO2 = (1.5703125, 4.83751296997e-04, 7.54978995489e-08)


def coords():
    b = lax.axis_index("blk")
    t = lax.axis_index("tp")
    return b, t, b // 4, (b // 2) % 2, b % 2, t // 4, t % 4


def blk_of(x, zl, c):
    return x * 4 + zl * 2 + c


def signal(dev):
    pl.semaphore_signal(pltpu.get_barrier_semaphore(), inc=1, device_id=dev, device_id_type=MESH)


def push(src, dst, ssem, rsem, dev):
    pltpu.make_async_remote_copy(src, dst, ssem, rsem, device_id=dev, device_id_type=MESH).start()


def landed(ref, sem):
    pltpu.make_async_copy(ref, ref, sem).wait()


def sends_of(pieces):
    return 15 * pieces


class Gather:
    def __init__(self, at, pieces, send, recv, xfirst=()):
        self.at, self.n, self.send, self.recv, self.xfirst = at, pieces, send, recv, xfirst
        b, t, x, zl, c, y, zh = coords()
        self.t = t
        self.own = b
        self.sib = blk_of(x, zl, 1 - c)
        self.z = blk_of(x, 1 - zl, c)
        xp, xm, x2 = (x + 1) % 4, (x + 3) % 4, (x + 2) % 4
        self.xp, self.xm = blk_of(xp, zl, c), blk_of(xm, zl, c)
        self.xpz, self.xmz = blk_of(xp, 1 - zl, c), blk_of(xm, 1 - zl, c)
        self.x2, self.x2z = blk_of(x2, zl, c), blk_of(x2, 1 - zl, c)
        self.order = (self.own, self.z, self.xm, self.xp, self.xmz, self.xpz, self.x2, self.x2z)
        self.count = 0
        self.sent = []

    def _send(self, chunk, p, to):
        ref = self.at(chunk, p)
        k = self.count
        self.count += 1
        push(ref, ref, self.send.at[k], self.recv.at[chunk, p], {"blk": to, "tp": self.t})
        self.sent.append((p, k))

    def wait(self, chunk, p):
        landed(self.at(chunk, p), self.recv.at[chunk, p])

    def own_z(self, *pieces):
        for p in pieces:
            for to in (self.z, self.sib):
                self._send(self.own, p, to)

    def own_x(self, *pieces):
        for p in pieces:
            for to in (self.xp, self.xm):
                self._send(self.own, p, to)

    def mine(self, *pieces):
        for p in pieces:
            self.own_x(p)
            self.own_z(p)

    def z_in(self, *pieces):
        for p in pieces:
            self.wait(self.z, p)
            self._send(self.z, p, self.sib)

    def z_out(self, *pieces):
        for p in pieces:
            for to in (self.xp, self.xm):
                self._send(self.z, p, to)

    def zfwd(self, *pieces):
        for p in pieces:
            self.wait(self.z, p)
            if p not in self.xfirst:
                self.z_out(p)
            self._send(self.z, p, self.sib)

    def side(self, zside, *pieces):
        minus, plus = (self.xmz, self.xpz) if zside else (self.xm, self.xp)
        for p in pieces:
            for chunk, on, even in ((minus, self.xp, 0), (plus, self.xm, 1)):
                self.wait(chunk, p)
                if p % 2 == even and not (zside and p in self.xfirst):
                    self._send(chunk, p, on)
                if p in self.xfirst and not zside:
                    self._send(chunk, p, self.z)
                self._send(chunk, p, self.sib)

    def far(self, zside, *pieces):
        chunk = self.x2z if zside else self.x2
        for p in pieces:
            self.wait(chunk, p)
            if p in self.xfirst and not zside:
                self._send(chunk, p, self.z)
            self._send(chunk, p, self.sib)

    def sibs(self, k):
        chunk = flip(self.order[k])
        for p in range(self.n):
            self.wait(chunk, p)

    def drain(self):
        for p, k in self.sent:
            landed(self.at(0, p), self.send.at[k])


def flip(k):
    return k + 1 - 2 * (k % 2)


def pick(options, i):
    r = options[0]
    for k in range(1, len(options)):
        r = jnp.where(i == k, options[k], r)
    return r


def run(n, compute, events):
    def body(i, carry):
        for k, event in events.items():
            pl.when(i == k)(event)
        compute(i)
        return carry

    lax.fori_loop(0, n, body, 0)


def seq(*calls):
    def go():
        for f, *args in calls:
            f(*args)

    return go


def cos_sin(angle):
    k = jnp.floor(angle * (2.0 / np.pi) + 0.5)
    r = ((angle - k * PIO2[0]) - k * PIO2[1]) - k * PIO2[2]
    s = r * r
    sin = r + r * s * (-1.6666654611e-1 + s * (8.3321608736e-3 + s * -1.9515295891e-4))
    cos = 1.0 - 0.5 * s + s * s * (4.166664568298827e-2 + s * (-1.388731625493765e-3 + s * 2.443315711809948e-5))
    m = k.astype(jnp.int32)
    odd = m % 2 == 1
    cos_v = jnp.where(odd, sin, cos)
    sin_v = jnp.where(odd, cos, sin)
    cos_v = jnp.where((m + 1) // 2 % 2 == 1, -cos_v, cos_v)
    sin_v = jnp.where(m // 2 % 2 == 1, -sin_v, sin_v)
    return cos_v, sin_v


def layer(
    dm, x_hbm, wq, wkv, wo, gain_h, qb_h, kb_h, pos_h, seg_h, freq_h,
    out,
    xv, slot, five, ordered, land, wide, w, land_o, wide_o, wog, segs, kaug, acc_w, trig, res, q, kvg, m_s, acc_s, cg,
    fb0, pb0, mb0, rf0, rp0, rm0, fb1, pb1, mb1, rf1, rp1, rm1,
    a_send, a_recv, o_send, o_recv, s_send, s_recv, g_send, g_recv, h_send, h_recv, k_send, k_recv, e_send, c_send, c_recv, p_send, p_recv,
    x_sem, gain, qb, kb, pos, seg, freq, gain_row, i_sem,
):
    b, t, x, zl, c, y, zh = coords()
    wide_bufs, narrow_bufs = (fb0, pb0, mb0, rf0, rp0, rm0), (fb1, pb1, mb1, rf1, rp1, rm1)
    hl = t % 2
    main = Gather(lambda k, p: w.at[k, pl.ds(pl.multiple_of((zh + p) % 4 * 80, 80), 80)], 4, g_send, g_recv)
    outw = Gather(lambda k, p: wog.at[k, :, pl.ds(p * 512, 512)], 2, h_send, h_recv)

    def kv_at(k, p):
        lane = pl.multiple_of(128 * ((hl + p // 2) % 2), 128)
        return kvg.at[k, pl.ds(256 * (p % 2), 256), pl.ds(lane, 128)]

    keys = Gather(kv_at, 4, k_send, k_recv, (3,))
    tgt_blk = blk_of(x, y // 2, y % 2)
    tgt_tp = [yb * 4 + 2 * zl + c for yb in range(4)]
    src_blk = blk_of(x, zh // 2, zh % 2)
    src_tp = [(2 * zl + c) * 4 + k for k in range(4)]

    def other(kb, kt):
        return jnp.logical_or(kb != b, kt != t)

    x_copy = pltpu.make_async_copy(x_hbm, xv, x_sem)
    x_copy.start()
    in_copy = [
        pltpu.make_async_copy(src, dst, i_sem.at[k])
        for k, (src, dst) in enumerate(((gain_h, gain), (qb_h, qb), (kb_h, kb), (pos_h, pos), (seg_h, seg), (freq_h, freq)))
    ]
    for copy in in_copy:
        copy.start()
    for k in range(1, 16):
        signal({"blk": b, "tp": (t + k) % 16})
        signal({"blk": (b + k) % 16, "tp": t})
    for k in range(4):
        @pl.when(other(tgt_blk, tgt_tp[k]))
        def _():
            signal({"blk": tgt_blk, "tp": tgt_tp[k]})

        @pl.when(other(src_blk, src_tp[k]))
        def _():
            signal({"blk": src_blk, "tp": src_tp[k]})
    loop = jnp.logical_and(y == 2 * zl + c, zh == 2 * zl + c).astype(jnp.int32)
    pl.semaphore_wait(pltpu.get_barrier_semaphore(), 38 - 2 * loop)

    def q_src(to):
        return wq.at[:, pl.ds(pl.multiple_of(to * 256, 256), 256)]

    def kv_src(to):
        return wkv.at[:, pl.ds(pl.multiple_of(to * 128, 128), 128)]

    def q_land(k):
        return land.at[k, :, pl.ds(0, 256)]

    def kv_land(k):
        return land.at[k, :, pl.ds(256, 128)]

    for k in range(1, 16):
        to = (y + k) % 4 * 4 + (zh + (0, 3, 1, 2)[k // 4]) % 4
        push(q_src(to), q_land(t), a_send.at[0, k], a_recv.at[0, t], {"blk": b, "tp": to})
        push(kv_src(to), kv_land(t), a_send.at[1, k], a_recv.at[1, t], {"blk": b, "tp": to})
    pltpu.make_async_copy(q_src(t), q_land(t), a_recv.at[0, t]).start()
    pltpu.make_async_copy(kv_src(t), kv_land(t), a_recv.at[1, t]).start()

    def send_segs():
        in_copy[4].wait()
        for k in range(1, 16):
            push(seg, segs.at[b], s_send.at[k], s_recv.at[b], {"blk": (b + k) % 16, "tp": t})
        segs[b] = seg[...]


    in_copy[0].wait()
    for k in range(D // 256):
        gain_row[:, k * 256 : (k + 1) * 256] = gain[k * 256 : (k + 1) * 256].astype(F32)[None, :]
    x_copy.wait()

    def squares(i, carry):
        rows = pl.ds(pl.multiple_of(i * 64, 64), 64)
        total = jnp.zeros((64, 128), F32)
        for j in range(D // 128):
            v = xv[rows, j * 128 : (j + 1) * 128].astype(F32)
            total = total + v * v
        square = jnp.maximum(jnp.sum(total, axis=1, keepdims=True) * (1.0 / D), NORM_FLOOR)
        trig[0, rows, :] = jnp.broadcast_to(lax.rsqrt(square), (64, 128))
        return carry

    lax.fori_loop(0, TOK // 64, squares, 0)

    def turn(i, carry):
        for k in range(5):
            at = pl.ds(pl.multiple_of(i * 640 + k * 128, 128), 128)
            v = xv[:, at].astype(F32) * trig[0] * gain_row[:, at]
            five[k * 128 : (k + 1) * 128, :] = v.astype(BF).astype(F32).T
        for k in range(32):
            slot[i * 32 + k] = five[k * ROWS : (k + 1) * ROWS, :]
        return carry

    lax.fori_loop(0, 8, turn, 0)

    def back(i):
        for k in range(32):
            f = k // 16 * 16 + k % 4 * 4 + k // 4 % 4
            five[k * ROWS : (k + 1) * ROWS, :] = slot[dm[i * 32 + f]]
        for k in range(5):
            ordered[:, k * 128 : (k + 1) * 128] = five[k * 128 : (k + 1) * 128, :].T.astype(BF)

    def group(g):
        zs = (zh + g) % 4
        for k in range(4):
            frm = 4 * k + zs
            landed(q_land(frm), a_recv.at[0, frm])
            landed(kv_land(frm), a_recv.at[1, frm])
            wide[k * ROWS : (k + 1) * ROWS, :] = land[frm].astype(F32)
        w[b, pl.ds(pl.multiple_of(zs * 80, 80), 80), :] = wide[...].astype(BF)
        main.mine(g)

    def send_out():
        for k in range(4):
            src = wo.at[:, pl.ds(k * 1024, 1024)]

            @pl.when(other(tgt_blk, tgt_tp[k]))
            def _():
                push(src, land_o.at[zh], o_send.at[k], o_recv.at[zh], {"blk": tgt_blk, "tp": tgt_tp[k]})

            @pl.when(jnp.logical_not(other(tgt_blk, tgt_tp[k])))
            def _():
                pltpu.make_async_copy(src, land_o.at[zh], o_recv.at[zh]).start()

    def squeeze_out():
        for k in range(4):
            landed(land_o.at[k], o_recv.at[k])
            wide_o[k * ROWS : (k + 1) * ROWS, :] = land_o[k].astype(F32)
        wog[b] = wide_o[...].astype(BF)
        outw.own_z(0, 1)

    group(0)
    group(1)
    main.zfwd(0)
    group(3)
    group(2)
    acc_w[...] = jnp.zeros((TOK, WC), F32)

    def rope_tables():
        for k in (1, 2, 3, 5):
            in_copy[k].wait()
        cos_t, sin_t = cos_sin(freq[...] * pos[...].astype(F32))
        trig[0] = jnp.concatenate([cos_t, cos_t], axis=0).T
        trig[1] = jnp.concatenate([-sin_t, sin_t], axis=0).T

    def mul(i):
        pair = pick(main.order, i) // 2
        back(pair)
        acc_w[...] += jnp.dot(ordered[...], w[pl.ds(pair * 2, 2)].reshape(640, WC), preferred_element_type=F32)

    run(8, mul, {
        0: seq((main.side, False, 0), (main.zfwd, 1), (main.sibs, 0)),
        1: seq((rope_tables,), (main.side, False, 1), (main.zfwd, 3), (main.zfwd, 2), (main.sibs, 1)),
        2: seq((send_segs,), (send_out,), (main.side, True, 0), (main.side, False, 3), (main.side, False, 2), (main.sibs, 2)),
        3: seq((main.far, False, 0), (main.side, True, 1), (main.sibs, 3)),
        4: seq((main.far, False, 1), (main.side, True, 3), (main.side, True, 2), (main.sibs, 4)),
        5: seq((main.far, False, 3), (main.far, False, 2), (main.sibs, 5)),
        6: seq((main.far, True, 0), (main.far, True, 1), (main.sibs, 6)),
        7: seq((main.far, True, 3), (main.far, True, 2), (main.sibs, 7)),
    })

    line = lax.broadcasted_iota(jnp.int32, (HD, TOK), 0)

    is_key = hl == 0
    kv_pair = kb[pl.ds(pl.multiple_of(t // 2 * 256, 256), 256)].astype(F32)[None, :]
    kv_bias = jnp.where(is_key, kv_pair[:, :HD], kv_pair[:, HD:])
    q_bias = qb[pl.ds(pl.multiple_of(t * 256, 256), 256)].astype(F32)[None, :]
    u = acc_w[:, 256:384] + kv_bias
    turned = u * trig[0] + pltpu.roll(u, HD // 2, 1) * trig[1]
    mine = pl.ds(pl.multiple_of(hl * 128, 128), 128)
    kvg[b, :, mine] = jnp.where(is_key, turned, u).astype(BF)
    partner = {"blk": b, "tp": t + 1 - 2 * hl}
    for r in range(2):
        push(kv_at(b, r), kv_at(b, r), e_send.at[r], k_recv.at[b, 2 + r], partner)
        keys.mine(r)
    own_seg = jnp.broadcast_to(seg[...].astype(F32), (HD, TOK))
    own_seg = jnp.where(line == 0, own_seg, jnp.where(line == 1, 1.0, 0.0)).T.astype(BF)
    for h in range(2):
        u = acc_w[:, h * HD : (h + 1) * HD] + q_bias[:, h * HD : (h + 1) * HD]
        u = (u * trig[0] + pltpu.roll(u, HD // 2, 1) * trig[1]).astype(BF)
        for r in range(2):
            q[r, h * 256 : (h + 1) * 256, 0:HD] = u[r * 256 : (r + 1) * 256]
            q[r, h * 256 : (h + 1) * 256, HD:] = own_seg[r * 256 : (r + 1) * 256]

    coef = HD ** -0.5 * LOG2E
    half = TOK // 2

    def column(j, carry):
        @pl.when(j != b)
        def _():
            landed(segs.at[j], s_recv.at[j])

        row = jnp.where(segs[j] == 0, NEGATIVE_FILL, 0.0)
        later = jnp.where(j // 2 > b // 2, NEGATIVE_FILL, 0.0)
        kaug[j] = jnp.where(
            line == 0, jnp.broadcast_to(row, (HD, TOK)), jnp.where(line == 1, later, 0.0)
        ).T.astype(BF)
        return carry

    lax.fori_loop(0, 16, column, 0)
    squeeze_out()
    window = pl.ds(pl.multiple_of(128 * ((5 * t) // 2), 128), 384)
    res[...] = xv[:, window].astype(F32).T

    def block(pair, r, first):
        ss = []
        for k in range(2):
            j = 2 * pair + k
            kop = jnp.concatenate([kvg[j, :, 0:HD], kaug[j]], axis=1)
            v = lax.dot_general(q[r], kop, (((1,), (1,)), ((), ())), preferred_element_type=F32)
            if first:
                qi = lax.broadcasted_iota(jnp.int32, (TOK, TOK), 0) % half + r * half + c * TOK
                ki = lax.broadcasted_iota(jnp.int32, (TOK, TOK), 1) + k * TOK
                v = jnp.where(ki <= qi, v, NEGATIVE_FILL)
            ss += [v[:, i * HD : (i + 1) * HD] for i in range(4)]
        top = ss
        while len(top) > 1:
            top = [jnp.maximum(top[i], top[i + 1]) for i in range(0, len(top), 2)]
        new = jnp.broadcast_to(jnp.max(top[0], axis=1, keepdims=True), (TOK, HD))
        if not first:
            old = m_s[r]
            new = jnp.maximum(old, new)
            factor = jnp.exp2((old - new) * coef)
        o = jnp.zeros((TOK, 2 * HD), F32)
        for k in range(2):
            e = jnp.concatenate([jnp.exp2((ss[4 * k + i] - new) * coef).astype(BF) for i in range(4)], axis=1)
            vop = jnp.concatenate([kvg[2 * pair + k, :, HD:], jnp.ones((TOK, HD), BF)], axis=1)
            o = o + jnp.dot(e, vop, preferred_element_type=F32)
        m_s[r] = new
        if first:
            acc_s[r] = o
        else:
            acc_s[r, :, 0:HD] = acc_s[r, :, 0:HD] * factor + o[:, 0:HD]
            acc_s[r, :, HD:] = acc_s[r, :, HD:] * factor + o[:, HD:]

    keys.side(False, 0, 1)
    for r in range(2):
        keys.wait(b, 2 + r)
        keys.mine(2 + r)
    keys.zfwd(0, 1)
    keys.sibs(0)
    block(b // 2, 0, True)
    block(b // 2, 1, True)
    keys.zfwd(2, 3)
    keys.side(False, 2, 3)
    keys.side(True, 0, 1)
    keys.sibs(1)

    @pl.when(keys.z < b)
    def _():
        block(keys.z // 2, 0, False)
        block(keys.z // 2, 1, False)

    def double(i):
        one = pick(keys.order[2::2], i % 3) // 2
        two = pick(keys.order[3::2], i % 3) // 2

        @pl.when(jnp.minimum(one, two) < b // 2)
        def _():
            block(one, i // 3, False)
            block(two, i // 3, False)

    up, down, opp = (zh + 1) % 4, (zh + 3) % 4, (zh + 2) % 4
    yp, ym, y2 = (y + 1) % 4, (y + 3) % 4, (y + 2) % 4
    zdev = lambda k: {"blk": b, "tp": y * 4 + k}
    ydev = lambda k: {"blk": b, "tp": k * 4 + zh}
    at = lambda k, p: cg.at[k, pl.ds(p * 64, 64)]
    part = TOK // 4

    def waitc(k, p):
        landed(at(k, p), c_recv.at[k, p])

    def mine_c(r):
        rows = pl.ds(r * half, half)
        for h in range(2):
            hr = pl.ds(h * half, half)
            cg[zh, rows, h * HD : (h + 1) * HD] = (acc_s[r, hr, 0:HD] / acc_s[r, hr, HD:]).astype(BF)
        for p in range(4 * r, 4 * r + 4):
            push(at(zh, p), at(zh, p), c_send.at[0, p], c_recv.at[zh, p], zdev(up))
            push(at(zh, p), at(zh, p), c_send.at[1, p], c_recv.at[zh, p], zdev(down))

    def fwd_c(*quarters):
        for r in quarters:
            waitc(down, 2 * r)
            push(at(down, 2 * r), at(down, 2 * r), c_send.at[2, 2 * r], c_recv.at[down, 2 * r], zdev(up))
            waitc(up, 2 * r + 1)
            push(at(up, 2 * r + 1), at(up, 2 * r + 1), c_send.at[2, 2 * r + 1], c_recv.at[up, 2 * r + 1], zdev(down))

    run(6, double, {
        0: seq((keys.side, True, 2), (keys.far, False, 0, 1), (keys.sibs, 2), (keys.sibs, 3)),
        1: seq((keys.side, True, 3), (outw.own_x, 0, 1), (keys.far, False, 2, 3), (keys.far, True, 0), (keys.sibs, 4), (keys.sibs, 5)),
        2: seq((outw.z_in, 0, 1), (outw.z_out, 0, 1), (keys.far, True, 1, 2, 3), (keys.sibs, 6), (keys.sibs, 7)),
        3: seq((mine_c, 0),),
        4: seq((outw.side, False, 0, 1)),
        5: seq((outw.side, True, 0, 1), (fwd_c, 0, 1)),
    })
    mine_c(1)
    outw.far(False, 0, 1)
    outw.far(True, 0, 1)
    for k in range(8):
        outw.sibs(k)

    parts = ((0, 256), (256, 128), (384, 128))
    far_b, plus, minus, r_far, r_plus, r_minus = [
        [wide_buf] + [narrow_buf.at[k] for k in range(2)]
        for wide_buf, narrow_buf in zip(wide_bufs, narrow_bufs)
    ]

    def partial(k, r):
        start, n = parts[r]
        v = jnp.zeros((320, n), F32)
        for i in range(4):
            v = v + lax.dot_general(
                wog[pl.ds(k * 4, 4), :, i * 256 : (i + 1) * 256].reshape(320, 256),
                cg[i, pl.ds(start, n), :],
                (((1,), (1,)), ((), ())),
                preferred_element_type=F32,
            )
        return v

    lo, hi = pl.ds(0, 160), pl.ds(160, 160)
    kept = {}

    def scatter_far(r):
        for k in ((0, 1), (2,), (3,))[r]:
            waitc(down, 2 * k + 1)
            waitc(up, 2 * k)
            waitc(opp, 2 * k)
            waitc(opp, 2 * k + 1)
        far_b[r][...] = partial(y2, r).astype(BF)
        push(far_b[r].at[lo], r_far[r].at[lo], p_send.at[r, 0], p_recv.at[r, 0], ydev(yp))
        push(far_b[r].at[hi], r_far[r].at[hi], p_send.at[r, 1], p_recv.at[r, 1], ydev(ym))

    def scatter_mid(r):
        v = partial(yp, r)
        plus[r][hi, :] = v[160:].astype(BF)
        push(plus[r].at[hi], r_plus[r].at[hi], p_send.at[r, 2], p_recv.at[r, 2], ydev(yp))
        u = partial(ym, r)
        minus[r][lo, :] = u[:160].astype(BF)
        push(minus[r].at[lo], r_minus[r].at[lo], p_send.at[r, 3], p_recv.at[r, 3], ydev(ym))
        kept[r] = v[:160], u[160:]

    def scatter_near(r):
        v, u = kept[r]
        landed(r_far[r].at[lo], p_recv.at[r, 0])
        plus[r][lo, :] = (v + r_far[r][lo, :].astype(F32)).astype(BF)
        push(plus[r].at[lo], r_plus[r].at[lo], p_send.at[r, 4], p_recv.at[r, 4], ydev(yp))
        landed(r_far[r].at[hi], p_recv.at[r, 1])
        minus[r][hi, :] = (u + r_far[r][hi, :].astype(F32)).astype(BF)
        push(minus[r].at[hi], r_minus[r].at[hi], p_send.at[r, 5], p_recv.at[r, 5], ydev(ym))

    def keep(r):
        cols = pl.ds(*parts[r])
        res[pl.ds(0, 320), cols] = partial(y, r) + res[pl.ds(pl.multiple_of(64 * hl, 64), 320), cols]

    def finish(r):
        for sl, k1, k2 in ((hi, 2, 5), (lo, 4, 3)):
            landed(r_plus[r].at[sl], p_recv.at[r, k1])
            landed(r_minus[r].at[sl], p_recv.at[r, k2])
        cols = pl.ds(*parts[r])
        out[:, cols] = (res[pl.ds(0, 320), cols] + r_plus[r][...].astype(F32) + r_minus[r][...].astype(F32)).astype(BF)

    scatter_far(0)
    scatter_mid(0)
    keep(0)
    fwd_c(2)
    fwd_c(3)
    scatter_near(0)
    scatter_far(1)
    scatter_far(2)
    scatter_mid(1)
    scatter_mid(2)
    scatter_near(1)
    keep(1)
    scatter_near(2)
    keep(2)
    finish(0)
    finish(1)
    finish(2)

    for k in range(1, 16):
        landed(q_land(0), a_send.at[0, k])
        landed(kv_land(0), a_send.at[1, k])
        landed(segs.at[0], s_send.at[k])
    for k in range(4):
        @pl.when(other(tgt_blk, tgt_tp[k]))
        def _():
            landed(land_o.at[k], o_send.at[k])

    for k in range(8):
        for i in range(3):
            landed(at(0, 0), c_send.at[i, k])
    for r in range(2):
        landed(kv_at(0, r), e_send.at[r])
    for r in range(3):
        for k in range(6):
            landed(far_b[r].at[lo], p_send.at[r, k])
    main.drain()
    outw.drain()
    keys.drain()


def per_device(residual_in, norm_gain, w_query, w_key_value, query_bias, key_value_bias, w_output, device_map, positions, segments):
    freq = (np.float64(ROPE_BASE) ** (-np.arange(HD // 2) * 2.0 / HD)).astype(np.float32)[:, None]
    freq = jnp.asarray(np.repeat(freq, TOK, axis=1))
    hbm = pl.BlockSpec(memory_space=pl.ANY)
    vm = pl.BlockSpec(memory_space=VM)
    turned = pl.pallas_call(
        layer,
        out_shape=jax.ShapeDtypeStruct((320, TOK), BF),
        in_specs=[pl.BlockSpec(memory_space=pltpu.SMEM), hbm, hbm, hbm, hbm, hbm, hbm, hbm, hbm, hbm, hbm],
        out_specs=vm,
        scratch_shapes=[
            VM((TOK, D), BF),
            VM((256, ROWS, TOK), F32),
            VM((640, TOK), F32),
            VM((TOK, 640), BF),
            VM((16, ROWS, WC), BF),
            VM((80, WC), F32),
            VM((16, 320, WC), BF),
            VM((4, ROWS, 1024), BF),
            VM((80, 1024), F32),
            VM((16, 80, 1024), BF),
            VM((16, 1, TOK), jnp.int32),
            VM((16, TOK, HD), BF),
            VM((TOK, WC), F32),
            VM((2, TOK, HD), F32),
            VM((384, TOK), F32),
            VM((2, TOK, 256), BF),
            VM((16, TOK, 256), BF),
            VM((2, TOK, HD), F32),
            VM((2, TOK, 256), F32),
            VM((4, TOK, 256), BF),
        ]
        + [VM((320, 256), BF)] * 6
        + [VM((2, 320, 128), BF)] * 6
        + [
            DMA((2, 16)), DMA((2, 16)), DMA((4,)), DMA((4,)), DMA((16,)), DMA((16,)),
            DMA((sends_of(4),)), DMA((16, 4)), DMA((sends_of(2),)), DMA((16, 2)), DMA((sends_of(4),)), DMA((16, 4)), DMA((2,)),
            DMA((3, 8)), DMA((4, 8)), DMA((3, 6)), DMA((3, 6)), DMA,
            VM((D,), BF), VM((4096,), BF), VM((2048,), BF), VM((1, TOK), jnp.int32), VM((1, TOK), jnp.int32), VM((HD // 2, TOK), F32), VM((1, D), F32),
            DMA((6,)),
        ],
        compiler_params=pltpu.CompilerParams(collective_id=0, has_side_effects=True, vmem_limit_bytes=VLIM),
        name="layer",
    )(
        device_map, residual_in, w_query, w_key_value, w_output.T, norm_gain, query_bias, key_value_bias,
        positions[None, :], segments[None, :], freq,
    )
    return turned.T


def solution(mesh):
    both = ("blk", "tp")
    placed = (P("blk", None), P(), P(both, None), P(both, None), P(), P(), P(None, both), P(), P("blk"), P("blk"))
    return jax.shard_map(per_device, mesh=mesh, in_specs=placed, out_specs=P("blk", "tp"), check_vma=False)
```
